768 devices in a mesh: box: 192 (over y, z, core), lev: 4 (over x).
Axes of the slice: x: 4, y: 8, z: 12, core: 2. Of those that a mesh axis runs over, the one named last changes fastest.
Arguments:
- fine: float32 [2304, 5, 32, 1024], P(('box', 'lev')), may hold values from -12 to 12
- coarse: float32 [5, 3072, 64, 128], P(None, 'box', 'lev'), may hold values from -6 to 6
- owner_map: int32 [2304, 2], P(('box', 'lev')), may hold values from -2 to 7, as said below
- patch_count: int32 [768], P(('box', 'lev')), may hold values from 1 to 3, as said below
- face_mask: int32 [2304, 6], P(('box', 'lev')), may hold values 0 or 1
Outputs:
- updated: float32 [5, 3072, 64, 128], P(None, 'box', 'lev')
- ghost: float32 [2304, 6, 5, 2048], P(('box', 'lev'))
The draws below stay inside these ranges and needn't reach their ends.
Inputs may be any that keep to these rules, and one draw needn't show every extreme that they name: `owner_map`: row p is fine patch p of device j = p // 3: column 0 is the offset k of its coarse owner, device (j + k) mod 768, one of -2, -1, 1, 2 and different for the 3 rows of one device; column 1 is a region r of that owner's block, 0 to 7. Rows of patches that are not live carry entries of the same kind and are ignored. No two live patches name the same owner and region. Device j holds live patches j * 3 to j * 3 + patch_count[j] - 1. Some device holds 3 live patches.
All inputs are finite; a program needn't handle non-finite values. No bound on the sum of `face_mask` on one device may be relied on, other than what follows from the above.
Results may differ from the reference program's by a relative error of at most 0.0003.
Values sent between devices are 32-bit elements; how exact they have to be, the bound alone decides.
No kernel may reach another device: no remote copies, remote signals or barrier semaphores. Data moves between devices by JAX's collectives and lax.ppermute only.
A program may use at most 128 MiB of HBM per device.

```python
import jax
import jax.numpy as jnp
from jax import lax

FIELDS = 5
F = 32
FPD = 3
R = 8
CZ = 128
NBLOCKS = 768
NFINE = 2304
NX = 3072
NY = 64
N_LEV = 4


def owner_table(key):
    first_key = jax.random.fold_in(key, 101)
    second_key = jax.random.fold_in(key, 202)
    base_offsets = jnp.tile(jnp.arange(4, dtype=jnp.int32), (NBLOCKS, 1))
    ordering = jax.random.permutation(first_key, base_offsets, axis=1, independent=True)[:, :FPD]
    delta_table = jnp.array([-2, -1, 1, 2], dtype=jnp.int32)
    offsets = delta_table[ordering]
    region_base = jnp.tile(jnp.arange(R, dtype=jnp.int32), (NBLOCKS, 1))
    region_perm = jax.random.permutation(second_key, region_base, axis=1, independent=True)
    target = (jnp.arange(NBLOCKS, dtype=jnp.int32)[:, None] + offsets) % NBLOCKS
    regions = region_perm[target, ordering]
    return jnp.stack([offsets.reshape(-1), regions.reshape(-1)], axis=1).astype(jnp.int32)


def draw_owner_map(key, part):
    return owner_table(key)


def draw_patch_count(key, part):
    counts = jax.random.randint(jax.random.fold_in(key, 7), (NBLOCKS,), 1, FPD + 1)
    fullest = jax.random.randint(jax.random.fold_in(key, 9), (), 0, NBLOCKS)
    return jnp.where(jnp.arange(NBLOCKS) == fullest, FPD, counts).astype(jnp.int32)


def touch_ends(values, own_key, smallest, top_value):
    spot = [jax.random.randint(jax.random.fold_in(own_key, axis), (), 0, length) for axis, length in enumerate(values.shape)]
    longest = values.shape.index(max(values.shape))
    next_to = spot[:longest] + [(spot[longest] + 1) % values.shape[longest]] + spot[longest + 1:]
    return values.at[tuple(spot)].set(smallest).at[tuple(next_to)].set(top_value)


def level_of(key, shape, cuts, low, high):
    def one(dim, blocks):
        draws = jax.random.uniform(jax.random.fold_in(jax.random.fold_in(key, 6), dim), (blocks,), jnp.float32, low / len(cuts), high / len(cuts))
        return jnp.repeat(jnp.exp(draws), shape[dim] // blocks).reshape((-1,) + (1,) * (len(shape) - dim - 1))

    level = one(*cuts[0])
    for cut in cuts[1:]:
        level = level * one(*cut)
    return level


def centred(stream_key, dims, scale, reach, shards=(), kind=jnp.bfloat16):
    factor_of = level_of(stream_key, dims, shards, -0.22, 0.18) if shards else 1.0
    entries = jax.random.normal(stream_key, dims, jnp.float32) * scale * factor_of
    return jnp.minimum(jnp.maximum(entries, -reach), reach).astype(kind)


def setup_inputs(seed: int = 0) -> dict:
    streams_of = jax.random.split(jax.random.key(seed), 6)
    fine = centred(streams_of[0], (NFINE, FIELDS, F, F * F), 2.0, 12.0, ((0, 768),), jnp.float32)
    coarse = centred(streams_of[1], (FIELDS, NX, NY, CZ), 1.0, 6.0, ((1, 192), (2, 4)), jnp.float32)
    owner_map = draw_owner_map(jax.random.fold_in(streams_of[5], 71), 0)
    patch_count = draw_patch_count(jax.random.fold_in(streams_of[5], 71), 0)
    face_mask = touch_ends((jax.random.randint(streams_of[4], (NFINE, 6), 0, 4) < 3).astype(jnp.int32), jax.random.fold_in(streams_of[4], 1), 0, 1)
    return {"fine": fine, "coarse": coarse, "owner_map": owner_map, "patch_count": patch_count, "face_mask": face_mask}


def restrict(fine):
    coarse_edge = fine.shape[2] // 2
    grouped = fine.reshape(fine.shape[0], fine.shape[1], coarse_edge, 2, coarse_edge, 2, coarse_edge, 2)
    return jnp.sum(grouped, axis=(3, 5, 7)) * 0.125


def widen(values):
    return jnp.repeat(jnp.repeat(jnp.repeat(values, 2, axis=1), 2, axis=2), 2, axis=3)


def interpolate(window):
    edge_cells = window.shape[1] - 4
    fine_width = 2 * edge_cells
    centre = window[:, 1:-1, 1:-1, 1:-1]
    slope_x = 0.5 * (window[:, 2:, 1:-1, 1:-1] - window[:, :-2, 1:-1, 1:-1])
    slope_y = 0.5 * (window[:, 1:-1, 2:, 1:-1] - window[:, 1:-1, :-2, 1:-1])
    slope_z = 0.5 * (window[:, 1:-1, 1:-1, 2:] - window[:, 1:-1, 1:-1, :-2])
    offset_sign = jnp.tile(jnp.array([-0.25, 0.25], dtype=window.dtype), edge_cells + 2)
    fine_value = (widen(centre) + offset_sign[None, :, None, None] * widen(slope_x)
                  + offset_sign[None, None, :, None] * widen(slope_y)
                  + offset_sign[None, None, None, :] * widen(slope_z))
    middle = slice(2, fine_width + 2)
    lower_rim = slice(0, 2)
    upper_rim = slice(fine_width + 2, fine_width + 4)
    face_list = [fine_value[:, lower_rim, middle, middle], fine_value[:, upper_rim, middle, middle],
                 fine_value[:, middle, lower_rim, middle], fine_value[:, middle, upper_rim, middle],
                 fine_value[:, middle, middle, lower_rim], fine_value[:, middle, middle, upper_rim]]
    return jnp.stack([each_face.reshape(each_face.shape[0], -1) for each_face in face_list])


def reference(fine, coarse, owner_map, patch_count, face_mask):
    coarse_edge = F // 2
    patch_total = fine.shape[0]
    per_device = patch_total // NBLOCKS
    averaged = restrict(fine)
    patch_ids = jnp.arange(patch_total, dtype=jnp.int32)
    holder = patch_ids // per_device
    is_live = (patch_ids % per_device) < patch_count[holder]
    target = (holder + owner_map[:, 0]) % NBLOCKS
    starts = jnp.stack([jnp.zeros_like(target), (target // N_LEV) * coarse_edge,
                        (target % N_LEV) * coarse_edge, owner_map[:, 1] * coarse_edge], axis=1).astype(jnp.int32)
    extent = (coarse.shape[0], coarse_edge, coarse_edge, coarse_edge)

    def write_patch(position, field):
        corner = [starts[position, 0], starts[position, 1], starts[position, 2], starts[position, 3]]
        present = lax.dynamic_slice(field, corner, extent)
        placed = jnp.where(is_live[position], averaged[position], present)
        return lax.dynamic_update_slice(field, placed, corner)

    updated = lax.fori_loop(0, patch_total, write_patch, coarse)
    padded = jnp.pad(updated, ((0, 0), (2, 2), (2, 2), (2, 2)), mode="wrap")
    window_extent = (coarse.shape[0], coarse_edge + 4, coarse_edge + 4, coarse_edge + 4)

    def ghost_of(position):
        corner = [starts[position, 0], starts[position, 1], starts[position, 2], starts[position, 3]]
        window = lax.dynamic_slice(padded, corner, window_extent)
        keep_mask = (is_live[position] & (face_mask[position] > 0)).astype(coarse.dtype)
        return interpolate(window) * keep_mask[:, None, None]

    ghosts = lax.map(ghost_of, patch_ids)
    return updated, ghosts
```

```python
import functools

import jax
import jax.numpy as jnp
from jax import lax
from jax.experimental import pallas as pl
from jax.experimental.pallas import tpu as pltpu
from jax.sharding import PartitionSpec as P


DELTAS = (-2, -1, 1, 2)
FIELDS = 5
E = 16
LANES = 128
PACK = 160
SHELL = 136
F32 = jnp.float32
BF16 = jnp.bfloat16


def split(x):
    hi = x.astype(BF16)
    lo = (x - hi.astype(F32)).astype(BF16)
    return hi, lo


def exact_dot(x, table):
    hi, lo = split(x)
    return jnp.dot(hi, table, preferred_element_type=F32) + jnp.dot(
        lo, table, preferred_element_type=F32
    )


def restrict_kernel(owner_ref, count_ref, fine_ref, *refs):
    out_refs, pair_ref = refs[:4], refs[4]
    slot = pl.program_id(0)

    @pl.when(slot == 0)
    def _():
        for out in out_refs:
            out[0:PACK, :] = jnp.zeros((PACK, LANES), F32)
            out[PACK : PACK + 8, :] = jnp.full((8, LANES), -1.0, F32)

    source = lax.broadcasted_iota(jnp.int32, (512, LANES), 0)
    target = lax.broadcasted_iota(jnp.int32, (512, LANES), 1)
    table = jnp.where((source // 64) * 16 + (source % 32) // 2 == target, 0.125, 0.0).astype(BF16)
    packed = []
    for g in range(2):
        pair_ref[...] = exact_dot(fine_ref[0, :, g * 512 : (g + 1) * 512], table)
        packed.append(pair_ref[pl.ds(0, 80, stride=2), :] + pair_ref[pl.ds(1, 80, stride=2), :])
    offset = owner_ref[0, slot]
    region = owner_ref[1, slot].astype(F32)
    live = slot < count_ref[0]
    for delta, out in zip(DELTAS, out_refs):

        @pl.when(live & (offset == delta))
        def _():
            for g in range(2):
                out[g * 80 : (g + 1) * 80, :] = packed[g]
            out[PACK : PACK + 8, :] = jnp.full((8, LANES), region, F32)


def label_of(ref, row):
    return jnp.max(ref[row : row + 8, :]).astype(jnp.int32)


def place_kernel(a0, a1, a2, a3, coarse_ref, upd_ref, low_ref, high_ref, label_ref):
    arrived = (a0, a1, a2, a3)
    labels = [label_of(a, PACK) for a in arrived]
    group = lax.broadcasted_iota(jnp.int32, (80, LANES), 1) // 16
    masks = [group == r for r in labels]
    for g in range(2):
        for i in range(8):
            rows = pl.ds(g * 8 + i, 80, stride=16)
            acc = coarse_ref[rows, :]
            for a, r, m in zip(arrived, labels, masks):
                shift = ((r - i) & 7) * 16
                acc = jnp.where(m, pltpu.roll(a[g * 80 : (g + 1) * 80, :], shift, 1), acc)
            upd_ref[rows, :] = acc
    for f in range(FIELDS):
        low_ref[f * 32 : f * 32 + 32, :] = upd_ref[f * 256 : f * 256 + 32, :]
        high_ref[f * 32 : f * 32 + 32, :] = upd_ref[f * 256 + 224 : f * 256 + 256, :]
    for k in range(4):
        label_ref[k * 8 : k * 8 + 8, :] = jnp.full((8, LANES), labels[k].astype(F32), F32)


def side_kernel(upd_ref, xl_ref, xh_ref, low_ref, high_ref):
    for out, near, far in ((low_ref, 0, 1), (high_ref, 15, 14)):
        out[160:176, :] = jnp.zeros((16, LANES), F32)
        out[0:80, :] = upd_ref[pl.ds(near, 80, stride=16), :]
        out[80:160, :] = upd_ref[pl.ds(far, 80, stride=16), :]
        out[160:165, :] = xl_ref[pl.ds(16 + near, 5, stride=32), :]
        out[168:173, :] = xh_ref[pl.ds(near, 5, stride=32), :]


def shell_kernel(label_ref, upd_ref, xl_ref, xh_ref, yl_ref, yh_ref, *refs):
    outs, z_ref = refs[:4], refs[4]
    labels = [jnp.maximum(label_of(label_ref, k * 8), 0) for k in range(4)]
    row = lax.broadcasted_iota(jnp.int32, (32, LANES), 0)
    lane = lax.broadcasted_iota(jnp.int32, (32, LANES), 1)
    layer = row % 6
    offset = jnp.where(layer < 3, layer - 2, layer + 12)
    base = jnp.zeros_like(row)
    for k in range(4):
        base = jnp.where(row // 6 == k, labels[k] * 16, base)
    pick = jnp.where((row < 24) & (((base + offset) & 127) == lane), 1.0, 0.0).astype(BF16)
    dims = (((1,), (1,)), ((), ()))
    for f in range(FIELDS):
        rows = jnp.concatenate(
            [
                upd_ref[f * 256 : f * 256 + 256, :],
                xl_ref[f * 32 + 16 : f * 32 + 32, :],
                xh_ref[f * 32 : f * 32 + 16, :],
                yl_ref[f * 16 : f * 16 + 16, :],
                yh_ref[f * 16 : f * 16 + 16, :],
            ],
            axis=0,
        )
        hi, lo = split(rows)
        picked = lax.dot_general(pick, hi, dims, preferred_element_type=F32) + lax.dot_general(
            pick, lo, dims, preferred_element_type=F32
        )
        for c, width in enumerate((LANES, LANES, 64)):
            at = c * 160 + f * 32
            z_ref[at : at + 32, 0:width] = picked[:, c * LANES : c * LANES + width]
    group = lax.broadcasted_iota(jnp.int32, (5, LANES), 1) // 16

    def put(k, tile, value):
        outs[k][tile * 5 : tile * 5 + 5, :] = value

    for k in range(4):
        for g in range(2):
            plane = [z_ref[pl.ds(g * 160 + k * 6 + n, 5, stride=32), :] for n in range(6)]
            put(k, 16 + g, plane[1])
            put(k, 18 + g, (plane[2] - plane[0]) * 0.125)
            put(k, 20 + g, plane[4])
            put(k, 22 + g, (plane[5] - plane[3]) * 0.125)
        first = z_ref[pl.ds(320 + k * 6 + 1, 5, stride=32), :]
        last = z_ref[pl.ds(320 + k * 6 + 4, 5, stride=32), :]
        put(k, 24, jnp.where(group < 4, first, pltpu.roll(last, 64, 1)))
        outs[k][130:136, :] = jnp.zeros((6, LANES), F32)

    def strip(q, t):
        if q == 0:
            p = xl_ref[pl.ds(16 + t, 5, stride=32), :]
            d = upd_ref[pl.ds(t, 5, stride=256), :] - xl_ref[pl.ds(t, 5, stride=32), :]
        elif q == 1:
            p = xh_ref[pl.ds(t, 5, stride=32), :]
            d = xh_ref[pl.ds(16 + t, 5, stride=32), :] - upd_ref[pl.ds(240 + t, 5, stride=256), :]
        elif q == 2:
            p = yl_ref[pl.ds(t, 5, stride=16), :]
            d = upd_ref[pl.ds(t * 16, 5, stride=256), :] - yl_ref[pl.ds(80 + t, 5, stride=16), :]
        else:
            p = yh_ref[pl.ds(t, 5, stride=16), :]
            d = (
                yh_ref[pl.ds(80 + t, 5, stride=16), :]
                - upd_ref[pl.ds(t * 16 + 15, 5, stride=256), :]
            )
        return p, d * 0.125

    for q in range(4):
        for g in range(2):
            accs = [[jnp.zeros((5, LANES), F32)] * 2 for _ in range(4)]
            for i in range(8):
                pd = strip(q, g * 8 + i)
                for k in range(4):
                    shift = ((i - labels[k]) & 7) * 16
                    accs[k] = [
                        jnp.where(group == i, pltpu.roll(v, shift, 1), a)
                        for v, a in zip(pd, accs[k])
                    ]
            for k in range(4):
                put(k, q * 4 + g, accs[k][0])
                put(k, q * 4 + 2 + g, accs[k][1])
    corners = (yl_ref[160:165, :], yh_ref[160:165, :], yl_ref[168:173, :], yh_ref[168:173, :])
    for k in range(4):
        acc = jnp.zeros((5, LANES), F32)
        for c in range(4):
            shift = ((c - labels[k]) & 7) * 16
            acc = jnp.where(group == c, pltpu.roll(corners[c], shift, 1), acc)
        put(k, 25, acc)


EDGES = (
    ((25, 0), (25, 1), (24, 0), (24, 4)),
    ((25, 2), (25, 3), (24, 1), (24, 5)),
    ((25, 0), (25, 2), (24, 2), (24, 6)),
    ((25, 1), (25, 3), (24, 3), (24, 7)),
    ((24, 0), (24, 1), (24, 2), (24, 3)),
    ((24, 4), (24, 5), (24, 6), (24, 7)),
)


def table_kernel(base_table, up_table):
    for chunk in range(8):
        cell = lax.broadcasted_iota(jnp.int32, (384, LANES), 0)
        col = lax.broadcasted_iota(jnp.int32, (384, LANES), 1) + chunk * LANES
        edge = (cell - 256) // 16
        along = cell % 16
        inside = cell < 256
        v = jnp.where(inside, cell // 16, jnp.where(edge == 0, -1, jnp.where(edge == 1, 16, along)))
        w = jnp.where(
            inside, along,
            jnp.where(edge < 2, along, jnp.where(edge == 2, -1, jnp.where(edge == 3, 16, -9))),
        )
        b = col // 32
        c = col % 32
        dv = v - b // 2
        dw = w - c // 2
        sb = jnp.where(b % 2 == 0, -0.125, 0.125)
        sc = jnp.where(c % 2 == 0, -0.125, 0.125)
        along_v = jnp.where(dv == 0, 1.0, jnp.where(dv == 1, sb, jnp.where(dv == -1, -sb, 0.0)))
        along_w = jnp.where(dw == 1, sc, jnp.where(dw == -1, -sc, 0.0))
        table = jnp.where(dw == 0, along_v, jnp.where(dv == 0, along_w, 0.0))
        lanes = slice(chunk * LANES, (chunk + 1) * LANES)
        base_table[:, lanes] = table.astype(BF16)
        up = jnp.where((dv == 0) & (dw == 0), 1.0, 0.0)
        up_table[0:256, lanes] = up[0:256].astype(BF16)
    k_at = lax.broadcasted_iota(jnp.int32, (256, 256), 0)
    n_at = lax.broadcasted_iota(jnp.int32, (256, 256), 1)
    from_y = ((n_at // 32) % 2) * 128 + (n_at // 64) * 32 + n_at % 32
    from_z = (n_at % 2) * 128 + n_at // 2
    up_table[256:512, 0:256] = jnp.where(k_at == from_y, 1.0, 0.0).astype(BF16)
    up_table[256:512, 256:512] = jnp.where(k_at == from_z, 1.0, 0.0).astype(BF16)
    up_table[256:512, 512:1024] = jnp.zeros((256, 512), BF16)


def ghost_kernel(owner_ref, count_ref, mask_ref, base_table, up_table, s0, s1, s2, s3, out_ref,
                 shell_ref, plane_ref):
    shells = (s0, s1, s2, s3)
    plane_ref[...] = jnp.zeros_like(plane_ref)
    group = lax.broadcasted_iota(jnp.int32, (5, LANES), 1) // 16
    for s in range(3):
        value = shells[0][...]
        for k in range(1, 4):
            value = jnp.where(owner_ref[0, s] == DELTAS[k], shells[k][...], value)
        shell_ref[...] = value
        for q in range(6):
            def rows(chunk):
                return pl.ds(chunk * 120 + s * 40 + q, 5, stride=8)

            for g in range(2):
                at = (q * 4 + g) * 5
                plane_ref[rows(g), :] = shell_ref[at : at + 5, :]
                plane_ref[rows(3 + g), :] = shell_ref[at + 10 : at + 15, :]
            edges = jnp.zeros((5, LANES), F32)
            for c, (tile, h) in enumerate(EDGES[q]):
                part = shell_ref[tile * 5 : tile * 5 + 5, :]
                shift = ((c - h) % 8) * 16
                if shift:
                    part = pltpu.roll(part, shift, 1)
                edges = jnp.where(group == c, part, edges)
            plane_ref[rows(2), :] = edges

    def chunks(first, count):
        return jnp.concatenate(
            [plane_ref[c * 120 : (c + 1) * 120, :] for c in range(first, first + count)], axis=1
        )

    base = exact_dot(chunks(0, 3), base_table[...])
    slope = exact_dot(chunks(3, 2), up_table[0:256, :])
    lower = base - slope
    upper = base + slope
    row = lax.broadcasted_iota(jnp.int32, (120, 256), 0)
    face = row % 8
    keep = jnp.zeros((120, 256), jnp.bool_)
    for s in range(3):
        for q in range(6):
            here = (row // 40 == s) & (face == q)
            keep = keep | (here & ((s < count_ref[0]) & (mask_ref[s, q] > 0)))
    for m in range(8):
        part = slice(m * LANES, (m + 1) * LANES)
        both = jnp.concatenate([lower[:, part], upper[:, part]], axis=1)
        along_y = exact_dot(both, up_table[256:512, 0:256])
        along_z = exact_dot(both, up_table[256:512, 256:512])
        along_x = (lower if m < 4 else upper)[:, (m % 4) * 256 : (m % 4 + 1) * 256]
        value = jnp.where(face < 2, along_x, jnp.where(face < 4, along_y, along_z))
        value = jnp.where(keep, value, 0.0)
        for s in range(3):
            for f in range(FIELDS):
                at = (s * 5 + f) * 8
                out_ref[s, f, :, m * 256 : (m + 1) * 256] = value[at : at + 6]


def vmem():
    return pl.BlockSpec(memory_space=pltpu.VMEM)


def smem():
    return pl.BlockSpec(memory_space=pltpu.SMEM)


def rows_of(n):
    return jax.ShapeDtypeStruct((n, LANES), F32)


def shift_axis(array, axis, by):
    size = lax.axis_size(axis)
    return lax.ppermute(array, axis, [(i, (i + by) % size) for i in range(size)])


def body(fine, coarse, owner_map, patch_count, face_mask):
    both = ("box", "lev")
    fine = fine.reshape(3, 160, 1024)
    coarse_rows = coarse.reshape(1280, LANES)
    owners = owner_map.T
    params = pltpu.CompilerParams(vmem_limit_bytes=16 << 20)
    slots = pl.pallas_call(
        restrict_kernel,
        compiler_params=params,
        grid=(3,),
        in_specs=[smem(), smem(), pl.BlockSpec((1, 160, 1024), lambda s: (s, 0, 0))],
        out_specs=[pl.BlockSpec((PACK + 8, LANES), lambda s: (0, 0))] * 4,
        out_shape=[rows_of(PACK + 8)] * 4,
        scratch_shapes=[pltpu.VMEM((160, LANES), F32)],
    )(owners, patch_count, fine)
    arrived = [shift_axis(a, both, d) for a, d in zip(slots, DELTAS)]
    updated, low, high, labels = pl.pallas_call(
        place_kernel,
        compiler_params=params,
        in_specs=[vmem()] * 5,
        out_specs=[vmem()] * 4,
        out_shape=[rows_of(1280), rows_of(160), rows_of(160), rows_of(32)],
    )(*arrived, coarse_rows)
    x_low = shift_axis(high, "box", 1)
    x_high = shift_axis(low, "box", -1)
    y_first, y_last = pl.pallas_call(
        side_kernel,
        compiler_params=params,
        in_specs=[vmem()] * 3,
        out_specs=[vmem()] * 2,
        out_shape=[rows_of(176)] * 2,
    )(updated, x_low, x_high)
    y_low = shift_axis(y_last, "lev", 1)
    y_high = shift_axis(y_first, "lev", -1)
    shells = pl.pallas_call(
        shell_kernel,
        compiler_params=params,
        in_specs=[vmem()] * 6,
        out_specs=[vmem()] * 4,
        out_shape=[rows_of(SHELL)] * 4,
        scratch_shapes=[pltpu.VMEM((480, LANES), F32)],
    )(labels, updated, x_low, x_high, y_low, y_high)
    back = [shift_axis(a, both, -d) for a, d in zip(shells, DELTAS)]
    tables = pl.pallas_call(
        table_kernel,
        compiler_params=params,
        out_specs=[vmem()] * 2,
        out_shape=[
            jax.ShapeDtypeStruct((384, 1024), BF16),
            jax.ShapeDtypeStruct((512, 1024), BF16),
        ],
    )()
    ghost = pl.pallas_call(
        ghost_kernel,
        compiler_params=params,
        in_specs=[smem()] * 3 + [vmem()] * 6,
        out_specs=vmem(),
        out_shape=jax.ShapeDtypeStruct((3, FIELDS, 6, 2048), F32),
        scratch_shapes=[pltpu.VMEM((SHELL, LANES), F32), pltpu.VMEM((600, LANES), F32)],
    )(owners, patch_count, face_mask, *tables, *back)
    ghost = jnp.transpose(ghost, (0, 2, 1, 3))
    return (updated.reshape(coarse.shape), ghost)


def solution(mesh):
    return jax.shard_map(
        body,
        mesh=mesh,
        in_specs=(
            P(("box", "lev"), None, None, None),
            P(None, "box", "lev", None),
            P(("box", "lev"), None),
            P(("box", "lev")),
            P(("box", "lev"), None),
        ),
        out_specs=(P(None, "box", "lev", None), P(("box", "lev"), None, None, None)),
        check_vma=False,
    )
```

```python
import functools

import jax
import jax.numpy as jnp
from jax import lax
from jax.experimental import pallas as pl
from jax.experimental.pallas import tpu as pltpu
from jax.sharding import PartitionSpec as P


DELTAS = (-2, -1, 1, 2)
FIELDS = 5
E = 16
LANES = 128
PACK = 160
SHELL = 136
F32 = jnp.float32
BF16 = jnp.bfloat16


def split(x):
    hi = x.astype(BF16)
    lo = (x - hi.astype(F32)).astype(BF16)
    return hi, lo


def exact_dot(x, table):
    hi, lo = split(x)
    return jnp.dot(hi, table, preferred_element_type=F32) + jnp.dot(
        lo, table, preferred_element_type=F32
    )


def carried_by(lev):
    return {-2: lev < 2, -1: lev == 0, 1: lev == 3, 2: lev >= 2}


def restrict_kernel(owner_ref, count_ref, fine_ref, own_ref, carry_ref, pair_ref):
    slot = pl.program_id(0)
    carried = carried_by(lax.axis_index("lev"))

    @pl.when(slot == 0)
    def _():
        own_ref[...] = jnp.zeros_like(own_ref)
        carry_ref[0 : 2 * PACK, :] = jnp.zeros((2 * PACK, LANES), F32)
        carry_ref[2 * PACK : 2 * PACK + 8, :] = jnp.full((8, LANES), -1.0, F32)

    source = lax.broadcasted_iota(jnp.int32, (512, LANES), 0)
    target = lax.broadcasted_iota(jnp.int32, (512, LANES), 1)
    table = jnp.where((source // 64) * 16 + (source % 32) // 2 == target, 0.125, 0.0).astype(BF16)
    packed = []
    for g in range(2):
        pair_ref[...] = exact_dot(fine_ref[0, :, g * 512 : (g + 1) * 512], table)
        packed.append(pair_ref[pl.ds(0, 80, stride=2), :] + pair_ref[pl.ds(1, 80, stride=2), :])
    offset = owner_ref[0, slot]
    region = owner_ref[1, slot].astype(F32)
    live = slot < count_ref[0]
    for n, delta in enumerate(DELTAS):
        here = live & (offset == delta)
        at = 0 if abs(delta) == 2 else 1

        @pl.when(here & carried[delta])
        def _():
            for g in range(2):
                row = at * PACK + g * 80
                carry_ref[row : row + 80, :] = packed[g]
            row = 2 * PACK + at * 4
            carry_ref[row : row + 4, :] = jnp.full((4, LANES), region, F32)

        @pl.when(here & jnp.logical_not(carried[delta]))
        def _():
            for g in range(2):
                row = n * PACK + g * 80
                own_ref[row : row + 80, :] = packed[g]


PIECES = (((1, 0), (-1, 1)), ((2, 0), (-2, 0)), ((-1, 0), (1, 1)), ((2, 1), (-2, 1)))
ROUTES = {1: (1, 0), -1: (3, 0), 2: (2, 0), -2: (2, 1)}
MESSAGE = 368


def message_kernel(owner_ref, count_ref, own_ref, carry_ref, coarse_ref, out_ref):
    lev = lax.axis_index("lev")
    carried = carried_by(lev)
    lane = lax.broadcasted_iota(jnp.int32, (8, LANES), 1)
    row8 = lax.broadcasted_iota(jnp.int32, (8, LANES), 0)
    carry_labels = carry_ref[2 * PACK : 2 * PACK + 8, :]
    data = {}
    label = {}
    for n, k in enumerate(DELTAS):
        at = 0 if abs(k) == 2 else 1
        data[k] = jnp.where(
            carried[k],
            carry_ref[at * PACK : (at + 1) * PACK, :],
            own_ref[n * PACK : (n + 1) * PACK, :],
        )
        mine = jnp.float32(-1.0)
        for s in range(3):
            here = (s < count_ref[0]) & (owner_ref[0, s] == k)
            mine = jnp.where(here, owner_ref[1, s].astype(F32), mine)
        label[k] = jnp.where(
            carried[k], jnp.where(row8 // 4 == at, carry_labels, -1.0), jnp.full((8, LANES), mine)
        )
        label[k] = jnp.max(label[k], axis=0, keepdims=True)
    starts = [pl.multiple_of(((lev + m) & 3) * MESSAGE, 8) for m in range(4)]
    for k in DELTAS:
        m, place = ROUTES[k]
        out_ref[pl.ds(starts[m] + place * PACK, PACK), :] = data[k]
    for m, layers in ((1, (15, 14)), (3, (0, 1))):
        for d, y in enumerate(layers):
            out_ref[pl.ds(starts[m] + PACK + d * 80, 80), :] = coarse_ref[pl.ds(y, 80, stride=16), :]
    none = jnp.full((1, LANES), -1.0, F32)
    wide = lax.broadcasted_iota(jnp.int32, (80, LANES), 1)
    for m in range(4):
        parts = []
        for n, (k, high) in enumerate(PIECES[m]):
            rows = data[k][80:160] if high else data[k][0:80]
            shift = 32 * (n + high)
            parts.append(pltpu.roll(rows, shift, 1) if shift else rows)
        tile = jnp.where(wide < 32, parts[0], parts[1])
        for f in range(FIELDS):
            near = tile[f * 16 : f * 16 + 8]
            far = pltpu.roll(tile[f * 16 + 8 : f * 16 + 16], 64, 1)
            out_ref[pl.ds(starts[m] + 320 + f * 8, 8), :] = jnp.where(lane < 64, near, far)
        first = label[1] if m == 1 else label[2] if m == 2 else label[-1] if m == 3 else none
        second = label[-2] if m == 2 else none
        k0, k1 = PIECES[m][0][0], PIECES[m][1][0]
        out_ref[pl.ds(starts[m] + 360, 8), :] = jnp.where(
            row8 < 2, first, jnp.where(row8 < 4, second, jnp.where(row8 < 6, label[k0], label[k1]))
        )


def label_of(ref, row):
    return jnp.max(ref[row : row + 8, :]).astype(jnp.int32)


def place_kernel(in_ref, coarse_ref, upd_ref, low_ref, high_ref, yl_ref, yh_ref, label_ref):
    lev = lax.axis_index("lev")
    starts = [pl.multiple_of(((lev - m) & 3) * MESSAGE, 8) for m in range(4)]
    row8 = lax.broadcasted_iota(jnp.int32, (8, LANES), 0)
    heads = [in_ref[pl.ds(starts[m] + 360, 8), :] for m in range(4)]

    def label(m, n):
        return jnp.max(jnp.where(row8 // 2 == n, heads[m], -1.0)).astype(jnp.int32)

    group = lax.broadcasted_iota(jnp.int32, (80, LANES), 1) // 16
    labels = [label(*ROUTES[k]) for k in DELTAS]
    masks = [group == r for r in labels]
    for g in range(2):
        arrived = [
            in_ref[pl.ds(starts[ROUTES[k][0]] + ROUTES[k][1] * PACK + g * 80, 80), :] for k in DELTAS
        ]
        for i in range(8):
            rows = pl.ds(g * 8 + i, 80, stride=16)
            acc = coarse_ref[rows, :]
            for a, r, m in zip(arrived, labels, masks):
                acc = jnp.where(m, pltpu.roll(a, ((r - i) & 7) * 16, 1), acc)
            upd_ref[rows, :] = acc
    for out, m_coarse, found in (
        (yl_ref, 1, ((0, 1), (2, 1), (3, 0), (3, 1))),
        (yh_ref, 3, ((0, 0), (2, 0), (1, 0), (1, 1))),
    ):
        high = out is yl_ref
        pieces = [(in_ref[pl.ds(starts[m] + 320, 40), :], n, label(m, n + 2)) for m, n in found]
        for d in range(2):
            halo = in_ref[pl.ds(starts[m_coarse] + PACK + d * 80, 80), :]
            for tile, n, r in pieces:
                first = n * 2 + (1 - d if high else d)
                halves = [
                    pltpu.roll(tile, ((r - first - h * 4) & 7) * 16, 1) for h in range(2)
                ]
                rows = []
                for f in range(FIELDS):
                    for h in range(2):
                        rows.append(halves[h][f * 8 : f * 8 + 8])
                halo = jnp.where(group == r, jnp.concatenate(rows, axis=0), halo)
            out[d * 80 : d * 80 + 80, :] = halo
    for out, x in ((low_ref, 0), (high_ref, 15)):
        step = 16 if x == 0 else -16
        for f in range(FIELDS):
            for d in range(2):
                at = f * 256 + x * 16 + d * step
                out[f * 32 + d * 16 : f * 32 + d * 16 + 16, :] = upd_ref[at : at + 16, :]
        out[160:176, :] = jnp.zeros((16, LANES), F32)
        out[160:165, :] = yl_ref[pl.ds(x, 5, stride=16), :]
        out[168:173, :] = yh_ref[pl.ds(x, 5, stride=16), :]
    for k in range(4):
        label_ref[k * 8 : k * 8 + 8, :] = jnp.full((8, LANES), labels[k].astype(F32), F32)


def shell_kernel(label_ref, upd_ref, xl_ref, xh_ref, yl_ref, yh_ref, *refs):
    outs, z_ref = refs[:4], refs[4]
    labels = [jnp.maximum(label_of(label_ref, k * 8), 0) for k in range(4)]
    row = lax.broadcasted_iota(jnp.int32, (32, LANES), 0)
    lane = lax.broadcasted_iota(jnp.int32, (32, LANES), 1)
    layer = row % 6
    offset = jnp.where(layer < 3, layer - 2, layer + 12)
    base = jnp.zeros_like(row)
    for k in range(4):
        base = jnp.where(row // 6 == k, labels[k] * 16, base)
    pick = jnp.where((row < 24) & (((base + offset) & 127) == lane), 1.0, 0.0).astype(BF16)
    dims = (((1,), (1,)), ((), ()))
    for f in range(FIELDS):
        rows = jnp.concatenate(
            [
                upd_ref[f * 256 : f * 256 + 256, :],
                xl_ref[f * 32 : f * 32 + 16, :],
                xh_ref[f * 32 : f * 32 + 16, :],
                yl_ref[f * 16 : f * 16 + 16, :],
                yh_ref[f * 16 : f * 16 + 16, :],
            ],
            axis=0,
        )
        hi, lo = split(rows)
        picked = lax.dot_general(pick, hi, dims, preferred_element_type=F32) + lax.dot_general(
            pick, lo, dims, preferred_element_type=F32
        )
        for c, width in enumerate((LANES, LANES, 64)):
            at = c * 160 + f * 32
            z_ref[at : at + 32, 0:width] = picked[:, c * LANES : c * LANES + width]
    group = lax.broadcasted_iota(jnp.int32, (5, LANES), 1) // 16

    def put(k, tile, value):
        outs[k][tile * 5 : tile * 5 + 5, :] = value

    for k in range(4):
        for g in range(2):
            plane = [z_ref[pl.ds(g * 160 + k * 6 + n, 5, stride=32), :] for n in range(6)]
            put(k, 16 + g, plane[1])
            put(k, 18 + g, (plane[2] - plane[0]) * 0.125)
            put(k, 20 + g, plane[4])
            put(k, 22 + g, (plane[5] - plane[3]) * 0.125)
        first = z_ref[pl.ds(320 + k * 6 + 1, 5, stride=32), :]
        last = z_ref[pl.ds(320 + k * 6 + 4, 5, stride=32), :]
        put(k, 24, jnp.where(group < 4, first, pltpu.roll(last, 64, 1)))
        outs[k][130:136, :] = jnp.zeros((6, LANES), F32)

    def strip(q, t):
        if q < 2:
            halo = xl_ref if q == 0 else xh_ref
            p = halo[pl.ds(t, 5, stride=32), :]
            far = halo[pl.ds(16 + t, 5, stride=32), :]
            inner = upd_ref[pl.ds(t + q * 240, 5, stride=256), :]
        else:
            halo = yl_ref if q == 2 else yh_ref
            p = halo[pl.ds(t, 5, stride=16), :]
            far = halo[pl.ds(80 + t, 5, stride=16), :]
            inner = upd_ref[pl.ds(t * 16 + (q - 2) * 15, 5, stride=256), :]
        d = far - inner if q % 2 else inner - far
        return p, d * 0.125

    for q in range(4):
        for g in range(2):
            accs = [[jnp.zeros((5, LANES), F32)] * 2 for _ in range(4)]
            for i in range(8):
                pd = strip(q, g * 8 + i)
                for k in range(4):
                    shift = ((i - labels[k]) & 7) * 16
                    accs[k] = [
                        jnp.where(group == i, pltpu.roll(v, shift, 1), a)
                        for v, a in zip(pd, accs[k])
                    ]
            for k in range(4):
                put(k, q * 4 + g, accs[k][0])
                put(k, q * 4 + 2 + g, accs[k][1])
    corners = (xl_ref[160:165, :], xl_ref[168:173, :], xh_ref[160:165, :], xh_ref[168:173, :])
    for k in range(4):
        acc = jnp.zeros((5, LANES), F32)
        for c in range(4):
            shift = ((c - labels[k]) & 7) * 16
            acc = jnp.where(group == c, pltpu.roll(corners[c], shift, 1), acc)
        put(k, 25, acc)


EDGES = (
    ((25, 0), (25, 1), (24, 0), (24, 4)),
    ((25, 2), (25, 3), (24, 1), (24, 5)),
    ((25, 0), (25, 2), (24, 2), (24, 6)),
    ((25, 1), (25, 3), (24, 3), (24, 7)),
    ((24, 0), (24, 1), (24, 2), (24, 3)),
    ((24, 4), (24, 5), (24, 6), (24, 7)),
)


def table_kernel(base_table, up_table):
    for chunk in range(8):
        cell = lax.broadcasted_iota(jnp.int32, (384, LANES), 0)
        col = lax.broadcasted_iota(jnp.int32, (384, LANES), 1) + chunk * LANES
        edge = (cell - 256) // 16
        along = cell % 16
        inside = cell < 256
        v = jnp.where(inside, cell // 16, jnp.where(edge == 0, -1, jnp.where(edge == 1, 16, along)))
        w = jnp.where(
            inside, along,
            jnp.where(edge < 2, along, jnp.where(edge == 2, -1, jnp.where(edge == 3, 16, -9))),
        )
        b = col // 32
        c = col % 32
        dv = v - b // 2
        dw = w - c // 2
        sb = jnp.where(b % 2 == 0, -0.125, 0.125)
        sc = jnp.where(c % 2 == 0, -0.125, 0.125)
        along_v = jnp.where(dv == 0, 1.0, jnp.where(dv == 1, sb, jnp.where(dv == -1, -sb, 0.0)))
        along_w = jnp.where(dw == 1, sc, jnp.where(dw == -1, -sc, 0.0))
        table = jnp.where(dw == 0, along_v, jnp.where(dv == 0, along_w, 0.0))
        lanes = slice(chunk * LANES, (chunk + 1) * LANES)
        base_table[:, lanes] = table.astype(BF16)
        up = jnp.where((dv == 0) & (dw == 0), 1.0, 0.0)
        up_table[0:256, lanes] = up[0:256].astype(BF16)
    k_at = lax.broadcasted_iota(jnp.int32, (256, 256), 0)
    n_at = lax.broadcasted_iota(jnp.int32, (256, 256), 1)
    from_y = ((n_at // 32) % 2) * 128 + (n_at // 64) * 32 + n_at % 32
    from_z = (n_at % 2) * 128 + n_at // 2
    up_table[256:512, 0:256] = jnp.where(k_at == from_y, 1.0, 0.0).astype(BF16)
    up_table[256:512, 256:512] = jnp.where(k_at == from_z, 1.0, 0.0).astype(BF16)
    up_table[256:512, 512:1024] = jnp.zeros((256, 512), BF16)


def ghost_kernel(owner_ref, count_ref, mask_ref, base_table, up_table, s0, s1, s2, s3, out_ref,
                 shell_ref, plane_ref):
    shells = (s0, s1, s2, s3)
    plane_ref[...] = jnp.zeros_like(plane_ref)
    group = lax.broadcasted_iota(jnp.int32, (5, LANES), 1) // 16
    for s in range(3):
        value = shells[0][...]
        for k in range(1, 4):
            value = jnp.where(owner_ref[0, s] == DELTAS[k], shells[k][...], value)
        shell_ref[...] = value
        for q in range(6):
            def rows(chunk):
                return pl.ds(chunk * 120 + s * 40 + q, 5, stride=8)

            for g in range(2):
                at = (q * 4 + g) * 5
                plane_ref[rows(g), :] = shell_ref[at : at + 5, :]
                plane_ref[rows(3 + g), :] = shell_ref[at + 10 : at + 15, :]
            edges = jnp.zeros((5, LANES), F32)
            for c, (tile, h) in enumerate(EDGES[q]):
                part = shell_ref[tile * 5 : tile * 5 + 5, :]
                shift = ((c - h) % 8) * 16
                if shift:
                    part = pltpu.roll(part, shift, 1)
                edges = jnp.where(group == c, part, edges)
            plane_ref[rows(2), :] = edges

    def chunks(first, count):
        return jnp.concatenate(
            [plane_ref[c * 120 : (c + 1) * 120, :] for c in range(first, first + count)], axis=1
        )

    base = exact_dot(chunks(0, 3), base_table[...])
    slope = exact_dot(chunks(3, 2), up_table[0:256, :])
    lower = base - slope
    upper = base + slope
    row = lax.broadcasted_iota(jnp.int32, (120, 256), 0)
    face = row % 8
    keep = jnp.zeros((120, 256), jnp.bool_)
    for s in range(3):
        for q in range(6):
            here = (row // 40 == s) & (face == q)
            keep = keep | (here & ((s < count_ref[0]) & (mask_ref[s, q] > 0)))
    for m in range(8):
        part = slice(m * LANES, (m + 1) * LANES)
        both = jnp.concatenate([lower[:, part], upper[:, part]], axis=1)
        along_y = exact_dot(both, up_table[256:512, 0:256])
        along_z = exact_dot(both, up_table[256:512, 256:512])
        along_x = (lower if m < 4 else upper)[:, (m % 4) * 256 : (m % 4 + 1) * 256]
        value = jnp.where(face < 2, along_x, jnp.where(face < 4, along_y, along_z))
        value = jnp.where(keep, value, 0.0)
        for s in range(3):
            for f in range(FIELDS):
                at = (s * 5 + f) * 8
                out_ref[s, f, :, m * 256 : (m + 1) * 256] = value[at : at + 6]


def vmem():
    return pl.BlockSpec(memory_space=pltpu.VMEM)


def smem():
    return pl.BlockSpec(memory_space=pltpu.SMEM)


def rows_of(n):
    return jax.ShapeDtypeStruct((n, LANES), F32)


def shift_axis(array, axis, by):
    size = lax.axis_size(axis)
    return lax.ppermute(array, axis, [(i, (i + by) % size) for i in range(size)])


def next_row(array):
    rows, levs = (lax.axis_size("box"), lax.axis_size("lev"))
    pairs = []
    for b in range(rows):
        for v in range(levs):
            by = 1 if v >= levs // 2 else -1
            pairs.append((b * levs + v, (b + by) % rows * levs + v))
    return lax.ppermute(array, ("box", "lev"), pairs)


def body(fine, coarse, owner_map, patch_count, face_mask):
    both = ("box", "lev")
    fine = fine.reshape(3, 160, 1024)
    coarse_rows = coarse.reshape(1280, LANES)
    owners = owner_map.T
    params = pltpu.CompilerParams(vmem_limit_bytes=16 << 20)
    own, leaving = pl.pallas_call(
        restrict_kernel,
        compiler_params=params,
        grid=(3,),
        in_specs=[smem(), smem(), pl.BlockSpec((1, 160, 1024), lambda s: (s, 0, 0))],
        out_specs=[
            pl.BlockSpec((4 * PACK, LANES), lambda s: (0, 0)),
            pl.BlockSpec((2 * PACK + 8, LANES), lambda s: (0, 0)),
        ],
        out_shape=[rows_of(4 * PACK), rows_of(2 * PACK + 8)],
        scratch_shapes=[pltpu.VMEM((160, LANES), F32)],
    )(owners, patch_count, fine)
    arriving = next_row(leaving)
    message = pl.pallas_call(
        message_kernel,
        compiler_params=params,
        in_specs=[smem()] * 2 + [vmem()] * 3,
        out_specs=vmem(),
        out_shape=rows_of(4 * MESSAGE),
    )(owners, patch_count, own, arriving, coarse_rows)
    received = lax.all_to_all(message.reshape(4, MESSAGE, LANES), "lev", 0, 0)
    updated, low, high, y_low, y_high, labels = pl.pallas_call(
        place_kernel,
        compiler_params=params,
        in_specs=[vmem()] * 2,
        out_specs=[vmem()] * 6,
        out_shape=[rows_of(n) for n in (1280, 176, 176, 160, 160, 32)],
    )(received.reshape(4 * MESSAGE, LANES), coarse_rows)
    x_low = shift_axis(high, "box", 1)
    x_high = shift_axis(low, "box", -1)
    shells = pl.pallas_call(
        shell_kernel,
        compiler_params=params,
        in_specs=[vmem()] * 6,
        out_specs=[vmem()] * 4,
        out_shape=[rows_of(SHELL)] * 4,
        scratch_shapes=[pltpu.VMEM((480, LANES), F32)],
    )(labels, updated, x_low, x_high, y_low, y_high)
    back = [shift_axis(a, both, -d) for a, d in zip(shells, DELTAS)]
    tables = pl.pallas_call(
        table_kernel,
        compiler_params=params,
        out_specs=[vmem()] * 2,
        out_shape=[
            jax.ShapeDtypeStruct((384, 1024), BF16),
            jax.ShapeDtypeStruct((512, 1024), BF16),
        ],
    )()
    ghost = pl.pallas_call(
        ghost_kernel,
        compiler_params=params,
        in_specs=[smem()] * 3 + [vmem()] * 6,
        out_specs=vmem(),
        out_shape=jax.ShapeDtypeStruct((3, FIELDS, 6, 2048), F32),
        scratch_shapes=[pltpu.VMEM((SHELL, LANES), F32), pltpu.VMEM((600, LANES), F32)],
    )(owners, patch_count, face_mask, *tables, *back)
    ghost = jnp.transpose(ghost, (0, 2, 1, 3))
    return (updated.reshape(coarse.shape), ghost)


def solution(mesh):
    return jax.shard_map(
        body,
        mesh=mesh,
        in_specs=(
            P(("box", "lev"), None, None, None),
            P(None, "box", "lev", None),
            P(("box", "lev"), None),
            P(("box", "lev")),
            P(("box", "lev"), None),
        ),
        out_specs=(P(None, "box", "lev", None), P(("box", "lev"), None, None, None)),
        check_vma=False,
    )
```

```python
import functools

import jax
import jax.numpy as jnp
from jax import lax
from jax.experimental import pallas as pl
from jax.experimental.pallas import tpu as pltpu
from jax.sharding import PartitionSpec as P


DELTAS = (-2, -1, 1, 2)
FIELDS = 5
E = 16
LANES = 128
PACK = 160
SHELL = 136
K1_VMEM = (64 << 20) - 900000
F32 = jnp.float32
BF16 = jnp.bfloat16


def split(x):
    hi = x.astype(BF16)
    lo = (x - hi.astype(F32)).astype(BF16)
    return hi, lo


def exact_dot(x, table):
    result = jnp.dot(jnp.concatenate(split(x), axis=0), table, preferred_element_type=F32)
    return result[: x.shape[0]] + result[x.shape[0] :]


def carried_by(lev):
    return {-2: lev < 2, -1: lev == 0, 1: lev == 3, 2: lev >= 2}


def restrict_kernel(owner_hbm, count_hbm, fine_hbm, own_ref, carry_ref,
                    fine_ref, owner_ref, count_ref, sems):
    loads = [
        pltpu.make_async_copy(
            fine_hbm.at[:, pl.ds(c * LANES, LANES)], fine_ref.at[pl.ds(c * 480, 480)], sems.at[c]
        )
        for c in range(8)
    ]
    small = [
        pltpu.make_async_copy(owner_hbm, owner_ref, sems.at[8]),
        pltpu.make_async_copy(count_hbm, count_ref, sems.at[9]),
    ]
    for copy in small + loads:
        copy.start()
    carried = carried_by(lax.axis_index("lev"))
    own_ref[0 : 4 * PACK, :] = jnp.zeros((4 * PACK, LANES), F32)
    own_ref[4 * PACK : 4 * PACK + 32, :] = jnp.full((32, LANES), -1.0, F32)
    carry_ref[0 : 2 * PACK, :] = jnp.zeros((2 * PACK, LANES), F32)
    carry_ref[2 * PACK : 2 * PACK + 8, :] = jnp.full((8, LANES), -1.0, F32)
    source = lax.broadcasted_iota(jnp.int32, (512, LANES), 0)
    target = lax.broadcasted_iota(jnp.int32, (512, LANES), 1)
    table = jnp.where((source // 64) * 16 + (source % 32) // 2 == target, 0.125, 0.0).astype(BF16)
    for copy in small:
        copy.wait()
    for g in range(2):
        pairs = []
        for c in range(4):
            loads[g * 4 + c].wait()
            at = (g * 4 + c) * 480
            pairs.append(
                fine_ref[pl.ds(at, 240, stride=2), :] + fine_ref[pl.ds(at + 1, 240, stride=2), :]
            )
        packed = exact_dot(jnp.concatenate(pairs, axis=1), table)
        for s in range(3):
            live = s < count_ref[0, 0]
            offset = owner_ref[0, s]
            part = packed[s * 80 : s * 80 + 80]
            for n, delta in enumerate(DELTAS):
                here = live & (offset == delta)
                at = 0 if abs(delta) == 2 else 1

                @pl.when(here & carried[delta])
                def _():
                    row = at * PACK + g * 80
                    carry_ref[row : row + 80, :] = part
                    if g == 0:
                        row = 2 * PACK + at * 4
                        region = owner_ref[1, s].astype(F32)
                        carry_ref[row : row + 4, :] = jnp.full((4, LANES), region, F32)

                @pl.when(here & jnp.logical_not(carried[delta]))
                def _():
                    row = n * PACK + g * 80
                    own_ref[row : row + 80, :] = part
                    if g == 0:
                        row = 4 * PACK + n * 8
                        region = owner_ref[1, s].astype(F32)
                        own_ref[row : row + 8, :] = jnp.full((8, LANES), region, F32)


PIECES = (((1, 0), (-1, 1)), ((2, 0), (-2, 0)), ((-1, 0), (1, 1)), ((2, 1), (-2, 1)))
ROUTES = {1: (1, 0), -1: (3, 0), 2: (2, 0), -2: (2, 1)}
MESSAGE = 368


def message_kernel(own_ref, carry_ref, coarse_ref, control_ref, out_ref):
    lev = lax.axis_index("lev")
    carried = carried_by(lev)
    lane = lax.broadcasted_iota(jnp.int32, (8, LANES), 1)
    row8 = lax.broadcasted_iota(jnp.int32, (8, LANES), 0)
    carry_labels = carry_ref[2 * PACK : 2 * PACK + 8, :]
    data = {}
    label = {}
    for n, k in enumerate(DELTAS):
        at = 0 if abs(k) == 2 else 1
        data[k] = jnp.where(
            carried[k],
            carry_ref[at * PACK : (at + 1) * PACK, :],
            own_ref[n * PACK : (n + 1) * PACK, :],
        )
        row = 4 * PACK + n * 8
        label[k] = jnp.where(
            carried[k],
            jnp.max(jnp.where(row8 // 4 == at, carry_labels, -1.0), axis=0, keepdims=True),
            own_ref[row : row + 1, :],
        )
    starts = [pl.multiple_of(((lev + m) & 3) * MESSAGE, 8) for m in range(4)]
    for k in DELTAS:
        m, place = ROUTES[k]
        out_ref[pl.ds(starts[m] + place * PACK, PACK), :] = data[k]
    for m, layers in ((1, (15, 14)), (3, (0, 1))):
        for d, y in enumerate(layers):
            out_ref[pl.ds(starts[m] + PACK + d * 80, 80), :] = coarse_ref[pl.ds(y, 80, stride=16), :]
    none = jnp.full((1, LANES), -1.0, F32)
    wide = lax.broadcasted_iota(jnp.int32, (80, LANES), 1)
    for m in range(4):
        parts = []
        for n, (k, high) in enumerate(PIECES[m]):
            rows = data[k][80:160] if high else data[k][0:80]
            shift = 32 * (n + high)
            parts.append(pltpu.roll(rows, shift, 1) if shift else rows)
        tile = jnp.where(wide < 32, parts[0], parts[1])
        for f in range(FIELDS):
            near = tile[f * 16 : f * 16 + 8]
            far = pltpu.roll(tile[f * 16 + 8 : f * 16 + 16], 64, 1)
            out_ref[pl.ds(starts[m] + 320 + f * 8, 8), :] = jnp.where(lane < 64, near, far)
        first = label[1] if m == 1 else label[2] if m == 2 else label[-1] if m == 3 else none
        second = label[-2] if m == 2 else none
        k0, k1 = PIECES[m][0][0], PIECES[m][1][0]
        out_ref[pl.ds(starts[m] + 360, 8), :] = jnp.where(
            row8 < 2, first, jnp.where(row8 < 4, second, jnp.where(row8 < 6, label[k0], label[k1]))
        )


PART = 112
HALO = 176
NT = (((1,), (1,)), ((), ()))


def pick_dot(pick, rows):
    hi, lo = split(rows)
    return lax.dot_general(pick, hi, NT, preferred_element_type=F32) + lax.dot_general(
        pick, lo, NT, preferred_element_type=F32
    )


def place_kernel(in_ref, coarse_ref, upd_hbm, back_ref, back2_ref, fwd_ref, part_ref,
                 upd_ref, yl_ref, yh_ref, z_ref, sem):
    lev = lax.axis_index("lev")
    rising = lev < 2
    starts = [pl.multiple_of(((lev - m) & 3) * MESSAGE, 8) for m in range(4)]
    row8 = lax.broadcasted_iota(jnp.int32, (8, LANES), 0)
    heads = [in_ref[pl.ds(starts[m] + 360, 8), :] for m in range(4)]

    def label(m, n):
        return jnp.max(jnp.where(row8 // 2 == n, heads[m], -1.0)).astype(jnp.int32)

    group = lax.broadcasted_iota(jnp.int32, (80, LANES), 1) // 16
    labels = [label(*ROUTES[k]) for k in DELTAS]
    masks = [group == r for r in labels]
    for g in range(2):
        arrived = [
            in_ref[pl.ds(starts[ROUTES[k][0]] + ROUTES[k][1] * PACK + g * 80, 80), :] for k in DELTAS
        ]
        for i in range(8):
            rows = pl.ds(g * 8 + i, 80, stride=16)
            acc = coarse_ref[rows, :]
            for a, r, m in zip(arrived, labels, masks):
                acc = jnp.where(m, pltpu.roll(a, ((r - i) & 7) * 16, 1), acc)
            upd_ref[rows, :] = acc
    store = pltpu.make_async_copy(upd_ref, upd_hbm, sem)
    store.start()

    @pl.when(lev < 4)
    def _():
        for out, m_coarse, found in (
            (yl_ref, 1, ((0, 1), (2, 1), (3, 0), (3, 1))),
            (yh_ref, 3, ((0, 0), (2, 0), (1, 0), (1, 1))),
        ):
            high = out is yl_ref
            pieces = [(in_ref[pl.ds(starts[m] + 320, 40), :], n, label(m, n + 2)) for m, n in found]
            for d in range(2):
                halo = in_ref[pl.ds(starts[m_coarse] + PACK + d * 80, 80), :]
                for tile, n, r in pieces:
                    first = n * 2 + (1 - d if high else d)
                    halves = [
                        pltpu.roll(tile, ((r - first - h * 4) & 7) * 16, 1) for h in range(2)
                    ]
                    rows = []
                    for f in range(FIELDS):
                        for h in range(2):
                            rows.append(halves[h][f * 8 : f * 8 + 8])
                    halo = jnp.where(group == r, jnp.concatenate(rows, axis=0), halo)
                out[d * 80 : d * 80 + 80, :] = halo
        for out, low in ((back2_ref, True), (fwd_ref, False)):
            at_low = rising if low else jnp.logical_not(rising)
            for f in range(FIELDS):
                for d in range(2):
                    one = upd_ref[f * 256 + d * 16 : f * 256 + d * 16 + 16, :]
                    two = upd_ref[f * 256 + 240 - d * 16 : f * 256 + 256 - d * 16, :]
                    out[f * 32 + d * 16 : f * 32 + d * 16 + 16, :] = jnp.where(at_low, one, two)
            out[160:176, :] = jnp.zeros((16, LANES), F32)
            for row, side in ((160, yl_ref), (168, yh_ref)):
                out[row : row + 5, :] = jnp.where(
                    at_low, side[pl.ds(0, 5, stride=16), :], side[pl.ds(15, 5, stride=16), :]
                )
        row = lax.broadcasted_iota(jnp.int32, (32, LANES), 0)
        lane = lax.broadcasted_iota(jnp.int32, (32, LANES), 1)
        layer = row % 6
        offset = jnp.where(layer < 3, layer - 2, layer + 12)
        base = jnp.zeros_like(row)
        for k in range(4):
            base = jnp.where(row // 6 == k, labels[k] * 16, base)
        pick = jnp.where((row < 24) & (((base + offset) & 127) == lane), 1.0, 0.0).astype(BF16)
        for f in range(FIELDS):
            rows = jnp.concatenate(
                [
                    upd_ref[f * 256 : f * 256 + 256, :],
                    yl_ref[f * 16 : f * 16 + 16, :],
                    yh_ref[f * 16 : f * 16 + 16, :],
                ],
                axis=0,
            )
            picked = pick_dot(pick, rows)
            for c, width in enumerate((LANES, LANES, 32)):
                at = c * 160 + f * 32
                z_ref[at : at + 32, 0:width] = picked[:, c * LANES : c * LANES + width]
        strip = lax.broadcasted_iota(jnp.int32, (5, LANES), 1) // 16

        def put(k, tile, value):
            at = k * PART + tile * 5
            part_ref[at : at + 5, :] = value

        for k in range(4):
            for g in range(2):
                plane = [z_ref[pl.ds(g * 160 + k * 6 + n, 5, stride=32), :] for n in range(6)]
                put(k, 8 + g, plane[1])
                put(k, 10 + g, (plane[0] - plane[2]) * 0.125)
                put(k, 12 + g, plane[4])
                put(k, 14 + g, (plane[5] - plane[3]) * 0.125)
            first = pltpu.roll(z_ref[pl.ds(320 + k * 6 + 1, 5, stride=32), :], 32, 1)
            last = pltpu.roll(z_ref[pl.ds(320 + k * 6 + 4, 5, stride=32), :], 96, 1)
            edge = jnp.where(strip // 2 == 1, first, jnp.where(strip // 2 == 3, last, 0.0))
            put(k, 16, edge)
            at = k * PART + 105
            part_ref[at : at + 7, :] = jnp.full((7, LANES), labels[k].astype(F32), F32)
        for q in range(2):
            side = yh_ref if q else yl_ref
            facing = fwd_ref if q else back2_ref
            for g in range(2):
                accs = [[jnp.zeros((5, LANES), F32)] * 3 for _ in range(4)]
                for i in range(8):
                    t = g * 8 + i
                    near = side[pl.ds(t, 5, stride=16), :]
                    far = side[pl.ds(80 + t, 5, stride=16), :]
                    inner = upd_ref[pl.ds(t * 16 + q * 15, 5, stride=256), :]
                    values = (near, (far - inner) * 0.125, facing[pl.ds(t, 5, stride=32), :])
                    for k in range(4):
                        shift = ((i - labels[k]) & 7) * 16
                        accs[k] = [
                            jnp.where(strip == i, pltpu.roll(v, shift, 1), a)
                            for v, a in zip(values, accs[k])
                        ]
                for k in range(4):
                    put(k, q * 4 + g, accs[k][0])
                    put(k, q * 4 + 2 + g, accs[k][1])
                    put(k, 17 + q * 2 + g, accs[k][2])
        back_ref[0:HALO, :] = back2_ref[...]
        for c, (up, down) in enumerate(((3, 0), (2, 1))):
            back_ref[HALO + c * PART : HALO + (c + 1) * PART, :] = jnp.where(
                rising,
                part_ref[up * PART : (up + 1) * PART, :],
                part_ref[down * PART : (down + 1) * PART, :],
            )

    store.wait()


def shell_kernel(part_ref, mine_ref, behind_ref, ahead_ref, beyond_ref, out_ref,
                 rear_ref, front_ref, edge_ref, pick_ref, shell_ref):
    lev = lax.axis_index("lev")
    rising = lev < 2
    falling = jnp.logical_not(rising)
    returned = (falling, lev == 3, lev == 0, rising)
    parts = []
    labels = []
    for n, k in enumerate(DELTAS):
        at = HALO + (0 if abs(k) == 2 else 1) * PART
        part = jnp.where(
            returned[n], ahead_ref[at : at + PART, :], part_ref[n * PART : (n + 1) * PART, :]
        )
        parts.append(part)
        labels.append(jnp.maximum(jnp.max(part[105:112]), 0.0).astype(jnp.int32))
        top = n * HALO
        rear_ref[top : top + HALO, :] = jnp.where(returned[n], mine_ref[...], behind_ref[...])
        front_ref[top : top + HALO, :] = jnp.where(
            returned[n], beyond_ref[...], ahead_ref[0:HALO, :]
        )
        for f in range(FIELDS):
            at = f * 128 + n * 32
            edge_ref[at : at + 16, :] = rear_ref[top + f * 32 : top + f * 32 + 16, :]
            edge_ref[at + 16 : at + 32, :] = front_ref[top + f * 32 : top + f * 32 + 16, :]
    row = lax.broadcasted_iota(jnp.int32, (8, LANES), 0)
    lane = lax.broadcasted_iota(jnp.int32, (8, LANES), 1)
    base = jnp.zeros_like(row)
    for k in range(4):
        base = jnp.where(row // 2 == k, labels[k] * 16, base)
    offset = jnp.where(row % 2 == 0, -1, 16)
    pick = jnp.where(((base + offset) & 127) == lane, 1.0, 0.0).astype(BF16)
    picked = pick_dot(pick, edge_ref[...])
    for f in range(FIELDS):
        pick_ref[f * 8 : f * 8 + 8, :] = picked[:, f * LANES : (f + 1) * LANES]
    group = lax.broadcasted_iota(jnp.int32, (5, LANES), 1) // 16
    for n, k in enumerate(DELTAS):
        top = n * HALO
        part = parts[n]
        r = labels[n]

        def put(tile, value):
            shell_ref[tile * 5 : tile * 5 + 5, :] = value

        shell_ref[0:80, :] = part[0:80]
        low = pltpu.roll(pick_ref[pl.ds(n * 2, 5, stride=8), :], (128 - n * 32) % 128, 1)
        high = pltpu.roll(pick_ref[pl.ds(n * 2 + 1, 5, stride=8), :], (192 - n * 32) % 128, 1)
        edge = jnp.where(group < 2, low, jnp.where(group // 2 == 2, high, part[80:85]))
        put(16, edge)
        for q, halo in enumerate((rear_ref, front_ref)):
            for g in range(2):
                near = jnp.zeros((5, LANES), F32)
                far = jnp.zeros((5, LANES), F32)
                for i in range(8):
                    t = top + g * 8 + i
                    shift = ((i - r) & 7) * 16
                    near = jnp.where(
                        group == i, pltpu.roll(halo[pl.ds(t, 5, stride=32), :], shift, 1), near
                    )
                    far = jnp.where(
                        group == i, pltpu.roll(halo[pl.ds(t + 16, 5, stride=32), :], shift, 1), far
                    )
                at = (17 + q * 2 + g) * 5
                put(17 + q * 4 + g, near)
                put(19 + q * 4 + g, (far - part[at : at + 5]) * 0.125)
        corners = (
            rear_ref[top + 160 : top + 165, :],
            rear_ref[top + 168 : top + 173, :],
            front_ref[top + 160 : top + 165, :],
            front_ref[top + 168 : top + 173, :],
        )
        acc = jnp.zeros((5, LANES), F32)
        for c in range(4):
            acc = jnp.where(group == c, pltpu.roll(corners[c], ((c - r) & 7) * 16, 1), acc)
        put(25, acc)
        shell_ref[130:136, :] = jnp.zeros((6, LANES), F32)
        m, place = ROUTES[-k]
        place = 1 if k == -2 else 0
        start = pl.multiple_of(((lev + m) & 3) * (2 * SHELL), 8)
        out_ref[pl.ds(start + place * SHELL, SHELL), :] = shell_ref[...]


EDGES = (
    ((25, 0), (25, 1), (16, 0), (16, 4)),
    ((25, 2), (25, 3), (16, 1), (16, 5)),
    ((25, 0), (25, 2), (16, 2), (16, 6)),
    ((25, 1), (25, 3), (16, 3), (16, 7)),
    ((16, 0), (16, 1), (16, 2), (16, 3)),
    ((16, 4), (16, 5), (16, 6), (16, 7)),
)


def table_kernel(owner_hbm, count_hbm, mask_hbm, base_table, up_table, control_ref,
                 owner_ref, count_ref, mask_ref, sems):
    loads = [
        pltpu.make_async_copy(source, target, sems.at[n])
        for n, (source, target) in enumerate(
            ((owner_hbm, owner_ref), (count_hbm, count_ref), (mask_hbm, mask_ref))
        )
    ]
    for load in loads:
        load.start()
    for chunk in range(8):
        cell = lax.broadcasted_iota(jnp.int32, (384, LANES), 0)
        col = lax.broadcasted_iota(jnp.int32, (384, LANES), 1) + chunk * LANES
        edge = (cell - 256) // 16
        along = cell % 16
        inside = cell < 256
        v = jnp.where(inside, cell // 16, jnp.where(edge == 0, -1, jnp.where(edge == 1, 16, along)))
        w = jnp.where(
            inside, along,
            jnp.where(edge < 2, along, jnp.where(edge == 2, -1, jnp.where(edge == 3, 16, -9))),
        )
        b = col // 32
        c = col % 32
        dv = v - b // 2
        dw = w - c // 2
        sb = jnp.where(b % 2 == 0, -0.125, 0.125)
        sc = jnp.where(c % 2 == 0, -0.125, 0.125)
        along_v = jnp.where(dv == 0, 1.0, jnp.where(dv == 1, sb, jnp.where(dv == -1, -sb, 0.0)))
        along_w = jnp.where(dw == 1, sc, jnp.where(dw == -1, -sc, 0.0))
        table = jnp.where(dw == 0, along_v, jnp.where(dv == 0, along_w, 0.0))
        lanes = slice(chunk * LANES, (chunk + 1) * LANES)
        base_table[:, lanes] = table.astype(BF16)
        up = jnp.where((dv == 0) & (dw == 0), 1.0, 0.0)
        up_table[0:256, lanes] = up[0:256].astype(BF16)
    k_at = lax.broadcasted_iota(jnp.int32, (256, 256), 0)
    n_at = lax.broadcasted_iota(jnp.int32, (256, 256), 1)
    from_y = ((n_at // 32) % 2) * 128 + (n_at // 64) * 32 + n_at % 32
    from_z = (n_at % 2) * 128 + n_at // 2
    up_table[256:512, 0:256] = jnp.where(k_at == from_y, 1.0, 0.0).astype(BF16)
    up_table[256:512, 256:512] = jnp.where(k_at == from_z, 1.0, 0.0).astype(BF16)
    up_table[256:512, 512:1024] = jnp.zeros((256, 512), BF16)
    for load in loads:
        load.wait()
    lev = lax.axis_index("lev")
    row = lax.broadcasted_iota(jnp.int32, (8, LANES), 0)
    for s in range(3):
        k = owner_ref[0, s]
        chosen = jnp.zeros((8, LANES), F32)
        for n, delta in enumerate(DELTAS):
            chosen = jnp.where((row == n) & (k == delta), 1.0, chosen)
        chosen = jnp.where((row == 4) & (((lev + k) & 3) < 2), 1.0, chosen)
        control_ref[s * 8 : s * 8 + 8, :] = chosen
        keep = jnp.zeros((8, LANES), F32)
        for q in range(6):
            keep = jnp.where(
                (row == q) & ((s < count_ref[0, 0]) & (mask_ref[s, q] > 0)), 1.0, keep
            )
        control_ref[24 + s * 8 : 32 + s * 8, :] = keep


def ghost_kernel(control_ref, base_table, up_table, in_ref, out_hbm,
                 shell_ref, plane_ref, spread_ref, out_ref, sems):
    lev = lax.axis_index("lev")
    plane_ref[...] = jnp.zeros_like(plane_ref)
    candidates = []
    for k in DELTAS:
        start = ((lev + k) & 3) * (2 * SHELL) + (SHELL if k == -2 else 0)
        candidates.append(in_ref[pl.ds(pl.multiple_of(start, 8), SHELL), :])
    group = lax.broadcasted_iota(jnp.int32, (5, LANES), 1) // 16
    for s in range(3):
        value = candidates[0]
        for n in range(1, 4):
            row = s * 8 + n
            value = jnp.where(control_ref[row : row + 1, :] > 0.5, candidates[n], value)
        shell_ref[...] = value
        rising = control_ref[s * 8 + 4 : s * 8 + 5, :] > 0.5
        tile = shell_ref[80:85, :]
        swapped = jnp.where(group % 4 == 0, pltpu.roll(tile, 112, 1), pltpu.roll(tile, 16, 1))
        shell_ref[80:85, :] = jnp.where(rising | (group % 4 > 1), tile, swapped)
        tile = shell_ref[125:130, :]
        swapped = jnp.where(group < 2, pltpu.roll(tile, 96, 1), pltpu.roll(tile, 32, 1))
        shell_ref[125:130, :] = jnp.where(rising, tile, swapped)
        for q in range(6):
            def rows(chunk):
                return pl.ds(chunk * 96 + q * 16 + s * 5, 5)

            def tile_at(n):
                if q >= 2:
                    at = ((q - 2) * 4 + n) * 5
                    return shell_ref[at : at + 5, :]
                one, two = ((17 + q * 4 + n) * 5, (21 - q * 4 + n) * 5)
                return jnp.where(rising, shell_ref[one : one + 5, :], shell_ref[two : two + 5, :])

            for g in range(2):
                slope = tile_at(2 + g)
                plane_ref[rows(g), :] = tile_at(g)
                plane_ref[rows(3 + g), :] = slope if q % 2 else -slope
            edges = jnp.zeros((5, LANES), F32)
            for c, (tile, h) in enumerate(EDGES[q]):
                part = shell_ref[tile * 5 : tile * 5 + 5, :]
                shift = ((c - h) % 8) * 16
                if shift:
                    part = pltpu.roll(part, shift, 1)
                edges = jnp.where(group == c, part, edges)
            plane_ref[rows(2), :] = edges

    def chunks(first, count):
        return jnp.concatenate(
            [plane_ref[c * 96 : (c + 1) * 96, :] for c in range(first, first + count)], axis=1
        )

    base = exact_dot(chunks(0, 3), base_table[...])
    slope = exact_dot(chunks(3, 2), up_table[0:256, :])
    lower = base - slope
    upper = base + slope
    keeps = [control_ref[24 + s * 8 : 30 + s * 8, :] > 0.5 for s in range(3)]
    stores = []
    for part in range(4):
        flat = (lower, upper)[part // 2]
        for q in range(2):
            for c in range(4):
                at = (part % 2) * 4 + c
                spread_ref[pl.ds(c * 8 + q, 15, stride=32), :] = flat[
                    q * 16 : q * 16 + 15, at * LANES : (at + 1) * LANES
                ]
        for first in (2, 4):
            top = first * 16
            both = []
            for m in range(part * 2, part * 2 + 2):
                lanes = slice(m * LANES, (m + 1) * LANES)
                both.append(
                    jnp.concatenate([lower[top : top + 32, lanes], upper[top : top + 32, lanes]], axis=1)
                )
            value = exact_dot(
                jnp.concatenate(both, axis=0), up_table[256:512, (first - 2) * 128 : first * 128]
            )
            for q in range(2):
                for c in range(4):
                    row = (c // 2) * 32 + q * 16
                    lanes = slice((c % 2) * LANES, (c % 2 + 1) * LANES)
                    spread_ref[pl.ds(c * 8 + first + q, 15, stride=32), :] = value[row : row + 15, lanes]
        for s in range(3):
            for f in range(FIELDS):
                for c in range(4):
                    row = (s * 5 + f) * 32 + c * 8
                    lanes = slice((part * 4 + c) * LANES, (part * 4 + c + 1) * LANES)
                    out_ref[s, f, :, lanes] = jnp.where(keeps[s], spread_ref[row : row + 6, :], 0.0)
        lanes = pl.ds(part * 512, 512)
        store = pltpu.make_async_copy(
            out_ref.at[:, :, :, lanes], out_hbm.at[:, :, :, lanes], sems.at[part]
        )
        store.start()
        stores.append(store)
    for store in stores:
        store.wait()


def vmem():
    return pl.BlockSpec(memory_space=pltpu.VMEM)


def hbm():
    return pl.BlockSpec(memory_space=pltpu.HBM)


def rows_of(n):
    return jax.ShapeDtypeStruct((n, LANES), F32)


def row_shift(array, by, upper_rises):
    rows, levs = (lax.axis_size("box"), lax.axis_size("lev"))
    pairs = []
    for b in range(rows):
        for v in range(levs):
            way = by if (v >= levs // 2) == upper_rises else -by
            pairs.append((b * levs + v, (b + way) % rows * levs + v))
    return lax.ppermute(array, ("box", "lev"), pairs)


def body(fine, coarse, owner_map, patch_count, face_mask):
    both = ("box", "lev")
    fine = fine.reshape(480, 1024)
    coarse_rows = coarse.reshape(1280, LANES)
    owners = owner_map.T
    counts = patch_count.reshape(1, 1)
    params = pltpu.CompilerParams(vmem_limit_bytes=16 << 20)
    own, leaving = pl.pallas_call(
        restrict_kernel,
        compiler_params=pltpu.CompilerParams(vmem_limit_bytes=K1_VMEM),
        in_specs=[hbm()] * 3,
        out_specs=[vmem()] * 2,
        out_shape=[rows_of(4 * PACK + 32), rows_of(2 * PACK + 8)],
        scratch_shapes=[
            pltpu.VMEM((8 * 480, LANES), F32),
            pltpu.SMEM((2, 3), jnp.int32),
            pltpu.SMEM((1, 1), jnp.int32),
            pltpu.SemaphoreType.DMA((10,)),
        ],
    )(owners, counts, fine)
    arriving = row_shift(leaving, 1, True)
    base_table, up_table, control = pl.pallas_call(
        table_kernel,
        compiler_params=params,
        in_specs=[hbm()] * 3,
        out_specs=[vmem()] * 3,
        out_shape=[
            jax.ShapeDtypeStruct((384, 1024), BF16),
            jax.ShapeDtypeStruct((512, 1024), BF16),
            rows_of(48),
        ],
        scratch_shapes=[
            pltpu.SMEM((2, 3), jnp.int32),
            pltpu.SMEM((1, 1), jnp.int32),
            pltpu.SMEM((3, 6), jnp.int32),
            pltpu.SemaphoreType.DMA((3,)),
        ],
    )(owners, counts, face_mask)
    message = pl.pallas_call(
        message_kernel,
        compiler_params=params,
        in_specs=[vmem()] * 4,
        out_specs=vmem(),
        out_shape=rows_of(4 * MESSAGE),
    )(own, arriving, coarse_rows, control)
    received = lax.all_to_all(message.reshape(4, MESSAGE, LANES), "lev", 0, 0)
    updated, back, back2, ahead, parts = pl.pallas_call(
        place_kernel,
        compiler_params=params,
        in_specs=[vmem()] * 2,
        out_specs=[hbm()] + [vmem()] * 4,
        out_shape=[rows_of(n) for n in (1280, HALO + 2 * PART, HALO, HALO, 4 * PART)],
        scratch_shapes=[pltpu.VMEM((n, LANES), F32) for n in (1280, 160, 160, 480)]
        + [pltpu.SemaphoreType.DMA],
    )(received.reshape(4 * MESSAGE, LANES), coarse_rows)
    from_beyond = row_shift(back2, -2, False)
    from_ahead = row_shift(back, -1, False)
    from_behind = row_shift(ahead, 1, False)
    shells = pl.pallas_call(
        shell_kernel,
        compiler_params=params,
        in_specs=[vmem()] * 5,
        out_specs=vmem(),
        out_shape=rows_of(8 * SHELL),
        scratch_shapes=[
            pltpu.VMEM((n, LANES), F32) for n in (4 * HALO, 4 * HALO, 640, 40, SHELL)
        ],
    )(parts, ahead, from_behind, from_ahead, from_beyond)
    returned = lax.all_to_all(shells.reshape(4, 2 * SHELL, LANES), "lev", 0, 0)
    ghost = pl.pallas_call(
        ghost_kernel,
        compiler_params=params,
        in_specs=[vmem()] * 4,
        out_specs=hbm(),
        out_shape=jax.ShapeDtypeStruct((3, FIELDS, 6, 2048), F32),
        scratch_shapes=[
            pltpu.VMEM((SHELL, LANES), F32),
            pltpu.VMEM((480, LANES), F32),
            pltpu.VMEM((480, LANES), F32),
            pltpu.VMEM((3, FIELDS, 6, 2048), F32),
            pltpu.SemaphoreType.DMA((4,)),
        ],
    )(control, base_table, up_table, returned.reshape(8 * SHELL, LANES))
    ghost = jnp.transpose(ghost, (0, 2, 1, 3))
    return (updated.reshape(coarse.shape), ghost)


def solution(mesh):
    return jax.shard_map(
        body,
        mesh=mesh,
        in_specs=(
            P(("box", "lev"), None, None, None),
            P(None, "box", "lev", None),
            P(("box", "lev"), None),
            P(("box", "lev")),
            P(("box", "lev"), None),
        ),
        out_specs=(P(None, "box", "lev", None), P(("box", "lev"), None, None, None)),
        check_vma=False,
    )
```

```python
import functools

import jax
import jax.numpy as jnp
from jax import lax
from jax.experimental import pallas as pl
from jax.experimental.pallas import tpu as pltpu
from jax.sharding import PartitionSpec as P


DELTAS = (-2, -1, 1, 2)
FIELDS = 5
E = 16
LANES = 128
PACK = 160
SHELL = 136
K1_VMEM = (64 << 20) - 12000000
F32 = jnp.float32
BF16 = jnp.bfloat16


def split(x):
    hi = x.astype(BF16)
    lo = (x - hi.astype(F32)).astype(BF16)
    return hi, lo


def exact_dot(x, table):
    result = jnp.dot(jnp.concatenate(split(x), axis=0), table, preferred_element_type=F32)
    return result[: x.shape[0]] + result[x.shape[0] :]


def carried_by(lev):
    return {-2: lev < 2, -1: lev == 0, 1: lev == 3, 2: lev >= 2}


def restrict_kernel(owner_hbm, count_hbm, fine_hbm, own_ref, carry_ref,
                    fine_ref, owner_ref, count_ref, sems):
    loads = [
        pltpu.make_async_copy(
            fine_hbm.at[:, pl.ds(c * LANES, LANES)], fine_ref.at[pl.ds(c * 480, 480)], sems.at[c]
        )
        for c in range(8)
    ]
    small = [
        pltpu.make_async_copy(owner_hbm, owner_ref, sems.at[8]),
        pltpu.make_async_copy(count_hbm, count_ref, sems.at[9]),
    ]
    for copy in small + loads:
        copy.start()
    carried = carried_by(lax.axis_index("lev"))
    own_ref[0 : 4 * PACK, :] = jnp.zeros((4 * PACK, LANES), F32)
    own_ref[4 * PACK : 4 * PACK + 32, :] = jnp.full((32, LANES), -1.0, F32)
    carry_ref[0 : 2 * PACK, :] = jnp.zeros((2 * PACK, LANES), F32)
    carry_ref[2 * PACK : 2 * PACK + 8, :] = jnp.full((8, LANES), -1.0, F32)
    source = lax.broadcasted_iota(jnp.int32, (512, LANES), 0)
    target = lax.broadcasted_iota(jnp.int32, (512, LANES), 1)
    table = jnp.where((source // 64) * 16 + (source % 32) // 2 == target, 0.125, 0.0).astype(BF16)
    for copy in small:
        copy.wait()
    for g in range(2):
        pairs = []
        for c in range(4):
            loads[g * 4 + c].wait()
            at = (g * 4 + c) * 480
            pairs.append(
                fine_ref[pl.ds(at, 240, stride=2), :] + fine_ref[pl.ds(at + 1, 240, stride=2), :]
            )
        packed = exact_dot(jnp.concatenate(pairs, axis=1), table)
        for s in range(3):
            live = s < count_ref[0, 0]
            offset = owner_ref[0, s]
            part = packed[s * 80 : s * 80 + 80]
            for n, delta in enumerate(DELTAS):
                here = live & (offset == delta)
                at = 0 if abs(delta) == 2 else 1

                @pl.when(here & carried[delta])
                def _():
                    row = at * PACK + g * 80
                    carry_ref[row : row + 80, :] = part
                    if g == 0:
                        row = 2 * PACK + at * 4
                        region = owner_ref[1, s].astype(F32)
                        carry_ref[row : row + 4, :] = jnp.full((4, LANES), region, F32)

                @pl.when(here & jnp.logical_not(carried[delta]))
                def _():
                    row = n * PACK + g * 80
                    own_ref[row : row + 80, :] = part
                    if g == 0:
                        row = 4 * PACK + n * 8
                        region = owner_ref[1, s].astype(F32)
                        own_ref[row : row + 8, :] = jnp.full((8, LANES), region, F32)


PIECES = (((1, 0), (-1, 1)), ((2, 0), (-2, 0)), ((-1, 0), (1, 1)), ((2, 1), (-2, 1)))
ROUTES = {1: (1, 0), -1: (3, 0), 2: (2, 0), -2: (2, 1)}
MESSAGE = 368


def message_kernel(own_ref, carry_ref, coarse_ref, control_ref, out_ref):
    lev = lax.axis_index("lev")
    carried = carried_by(lev)
    lane = lax.broadcasted_iota(jnp.int32, (8, LANES), 1)
    row8 = lax.broadcasted_iota(jnp.int32, (8, LANES), 0)
    carry_labels = carry_ref[2 * PACK : 2 * PACK + 8, :]
    data = {}
    label = {}
    for n, k in enumerate(DELTAS):
        at = 0 if abs(k) == 2 else 1
        data[k] = jnp.where(
            carried[k],
            carry_ref[at * PACK : (at + 1) * PACK, :],
            own_ref[n * PACK : (n + 1) * PACK, :],
        )
        row = 4 * PACK + n * 8
        label[k] = jnp.where(
            carried[k],
            jnp.max(jnp.where(row8 // 4 == at, carry_labels, -1.0), axis=0, keepdims=True),
            own_ref[row : row + 1, :],
        )
    starts = [pl.multiple_of(((lev + m) & 3) * MESSAGE, 8) for m in range(4)]
    for k in DELTAS:
        m, place = ROUTES[k]
        out_ref[pl.ds(starts[m] + place * PACK, PACK), :] = data[k]
    for m, layers in ((1, (15, 14)), (3, (0, 1))):
        for d, y in enumerate(layers):
            out_ref[pl.ds(starts[m] + PACK + d * 80, 80), :] = coarse_ref[pl.ds(y, 80, stride=16), :]
    none = jnp.full((1, LANES), -1.0, F32)
    wide = lax.broadcasted_iota(jnp.int32, (80, LANES), 1)
    for m in range(4):
        parts = []
        for n, (k, high) in enumerate(PIECES[m]):
            rows = data[k][80:160] if high else data[k][0:80]
            shift = 32 * (n + high)
            parts.append(pltpu.roll(rows, shift, 1) if shift else rows)
        tile = jnp.where(wide < 32, parts[0], parts[1])
        for f in range(FIELDS):
            near = tile[f * 16 : f * 16 + 8]
            far = pltpu.roll(tile[f * 16 + 8 : f * 16 + 16], 64, 1)
            out_ref[pl.ds(starts[m] + 320 + f * 8, 8), :] = jnp.where(lane < 64, near, far)
        first = label[1] if m == 1 else label[2] if m == 2 else label[-1] if m == 3 else none
        second = label[-2] if m == 2 else none
        k0, k1 = PIECES[m][0][0], PIECES[m][1][0]
        out_ref[pl.ds(starts[m] + 360, 8), :] = jnp.where(
            row8 < 2, first, jnp.where(row8 < 4, second, jnp.where(row8 < 6, label[k0], label[k1]))
        )


PART = 112
HALO = 176
NT = (((1,), (1,)), ((), ()))


def pick_dot(pick, rows):
    hi, lo = split(rows)
    return lax.dot_general(pick, hi, NT, preferred_element_type=F32) + lax.dot_general(
        pick, lo, NT, preferred_element_type=F32
    )


def place_kernel(in_ref, coarse_ref, upd_hbm, back_ref, back2_ref, fwd_ref, part_ref,
                 upd_ref, yl_ref, yh_ref, z_ref, sem):
    lev = lax.axis_index("lev")
    rising = lev < 2
    starts = [pl.multiple_of(((lev - m) & 3) * MESSAGE, 8) for m in range(4)]
    row8 = lax.broadcasted_iota(jnp.int32, (8, LANES), 0)
    heads = [in_ref[pl.ds(starts[m] + 360, 8), :] for m in range(4)]

    def label(m, n):
        return jnp.max(jnp.where(row8 // 2 == n, heads[m], -1.0)).astype(jnp.int32)

    group = lax.broadcasted_iota(jnp.int32, (80, LANES), 1) // 16
    labels = [label(*ROUTES[k]) for k in DELTAS]
    masks = [group == r for r in labels]
    for g in range(2):
        arrived = [
            in_ref[pl.ds(starts[ROUTES[k][0]] + ROUTES[k][1] * PACK + g * 80, 80), :] for k in DELTAS
        ]
        for i in range(8):
            rows = pl.ds(g * 8 + i, 80, stride=16)
            acc = coarse_ref[rows, :]
            for a, r, m in zip(arrived, labels, masks):
                acc = jnp.where(m, pltpu.roll(a, ((r - i) & 7) * 16, 1), acc)
            upd_ref[rows, :] = acc
    store = pltpu.make_async_copy(upd_ref, upd_hbm, sem)
    store.start()

    @pl.when(lev < 4)
    def _():
        for out, m_coarse, found in (
            (yl_ref, 1, ((0, 1), (2, 1), (3, 0), (3, 1))),
            (yh_ref, 3, ((0, 0), (2, 0), (1, 0), (1, 1))),
        ):
            high = out is yl_ref
            pieces = [(in_ref[pl.ds(starts[m] + 320, 40), :], n, label(m, n + 2)) for m, n in found]
            for d in range(2):
                halo = in_ref[pl.ds(starts[m_coarse] + PACK + d * 80, 80), :]
                for tile, n, r in pieces:
                    first = n * 2 + (1 - d if high else d)
                    halves = [
                        pltpu.roll(tile, ((r - first - h * 4) & 7) * 16, 1) for h in range(2)
                    ]
                    rows = []
                    for f in range(FIELDS):
                        for h in range(2):
                            rows.append(halves[h][f * 8 : f * 8 + 8])
                    halo = jnp.where(group == r, jnp.concatenate(rows, axis=0), halo)
                out[d * 80 : d * 80 + 80, :] = halo
        for out, low in ((back2_ref, True), (fwd_ref, False)):
            at_low = rising if low else jnp.logical_not(rising)
            for f in range(FIELDS):
                for d in range(2):
                    one = upd_ref[f * 256 + d * 16 : f * 256 + d * 16 + 16, :]
                    two = upd_ref[f * 256 + 240 - d * 16 : f * 256 + 256 - d * 16, :]
                    out[f * 32 + d * 16 : f * 32 + d * 16 + 16, :] = jnp.where(at_low, one, two)
            out[160:176, :] = jnp.zeros((16, LANES), F32)
            for row, side in ((160, yl_ref), (168, yh_ref)):
                out[row : row + 5, :] = jnp.where(
                    at_low, side[pl.ds(0, 5, stride=16), :], side[pl.ds(15, 5, stride=16), :]
                )
        row = lax.broadcasted_iota(jnp.int32, (32, LANES), 0)
        lane = lax.broadcasted_iota(jnp.int32, (32, LANES), 1)
        layer = row % 6
        offset = jnp.where(layer < 3, layer - 2, layer + 12)
        base = jnp.zeros_like(row)
        for k in range(4):
            base = jnp.where(row // 6 == k, labels[k] * 16, base)
        pick = jnp.where((row < 24) & (((base + offset) & 127) == lane), 1.0, 0.0).astype(BF16)
        for f in range(FIELDS):
            rows = jnp.concatenate(
                [
                    upd_ref[f * 256 : f * 256 + 256, :],
                    yl_ref[f * 16 : f * 16 + 16, :],
                    yh_ref[f * 16 : f * 16 + 16, :],
                ],
                axis=0,
            )
            picked = pick_dot(pick, rows)
            for c, width in enumerate((LANES, LANES, 32)):
                at = c * 160 + f * 32
                z_ref[at : at + 32, 0:width] = picked[:, c * LANES : c * LANES + width]
        strip = lax.broadcasted_iota(jnp.int32, (5, LANES), 1) // 16

        def put(k, tile, value):
            at = k * PART + tile * 5
            part_ref[at : at + 5, :] = value

        for k in range(4):
            for g in range(2):
                plane = [z_ref[pl.ds(g * 160 + k * 6 + n, 5, stride=32), :] for n in range(6)]
                put(k, 8 + g, plane[1])
                put(k, 10 + g, (plane[0] - plane[2]) * 0.125)
                put(k, 12 + g, plane[4])
                put(k, 14 + g, (plane[5] - plane[3]) * 0.125)
            first = pltpu.roll(z_ref[pl.ds(320 + k * 6 + 1, 5, stride=32), :], 32, 1)
            last = pltpu.roll(z_ref[pl.ds(320 + k * 6 + 4, 5, stride=32), :], 96, 1)
            edge = jnp.where(strip // 2 == 1, first, jnp.where(strip // 2 == 3, last, 0.0))
            put(k, 16, edge)
            at = k * PART + 105
            part_ref[at : at + 7, :] = jnp.full((7, LANES), labels[k].astype(F32), F32)
        for q in range(2):
            side = yh_ref if q else yl_ref
            facing = fwd_ref if q else back2_ref
            for g in range(2):
                accs = [[jnp.zeros((5, LANES), F32)] * 3 for _ in range(4)]
                for i in range(8):
                    t = g * 8 + i
                    near = side[pl.ds(t, 5, stride=16), :]
                    far = side[pl.ds(80 + t, 5, stride=16), :]
                    inner = upd_ref[pl.ds(t * 16 + q * 15, 5, stride=256), :]
                    values = (near, (far - inner) * 0.125, facing[pl.ds(t, 5, stride=32), :])
                    for k in range(4):
                        shift = ((i - labels[k]) & 7) * 16
                        accs[k] = [
                            jnp.where(strip == i, pltpu.roll(v, shift, 1), a)
                            for v, a in zip(values, accs[k])
                        ]
                for k in range(4):
                    put(k, q * 4 + g, accs[k][0])
                    put(k, q * 4 + 2 + g, accs[k][1])
                    put(k, 17 + q * 2 + g, accs[k][2])
        back_ref[0:HALO, :] = back2_ref[...]
        for c, (up, down) in enumerate(((3, 0), (2, 1))):
            back_ref[HALO + c * PART : HALO + (c + 1) * PART, :] = jnp.where(
                rising,
                part_ref[up * PART : (up + 1) * PART, :],
                part_ref[down * PART : (down + 1) * PART, :],
            )

    store.wait()


def shell_kernel(part_ref, mine_ref, behind_ref, ahead_ref, beyond_ref, out_ref,
                 rear_ref, front_ref, edge_ref, pick_ref, shell_ref):
    lev = lax.axis_index("lev")
    rising = lev < 2
    falling = jnp.logical_not(rising)
    returned = (falling, lev == 3, lev == 0, rising)
    parts = []
    labels = []
    for n, k in enumerate(DELTAS):
        at = HALO + (0 if abs(k) == 2 else 1) * PART
        part = jnp.where(
            returned[n], ahead_ref[at : at + PART, :], part_ref[n * PART : (n + 1) * PART, :]
        )
        parts.append(part)
        labels.append(jnp.maximum(jnp.max(part[105:112]), 0.0).astype(jnp.int32))
        top = n * HALO
        rear_ref[top : top + HALO, :] = jnp.where(returned[n], mine_ref[...], behind_ref[...])
        front_ref[top : top + HALO, :] = jnp.where(
            returned[n], beyond_ref[...], ahead_ref[0:HALO, :]
        )
        for f in range(FIELDS):
            at = f * 128 + n * 32
            edge_ref[at : at + 16, :] = rear_ref[top + f * 32 : top + f * 32 + 16, :]
            edge_ref[at + 16 : at + 32, :] = front_ref[top + f * 32 : top + f * 32 + 16, :]
    row = lax.broadcasted_iota(jnp.int32, (8, LANES), 0)
    lane = lax.broadcasted_iota(jnp.int32, (8, LANES), 1)
    base = jnp.zeros_like(row)
    for k in range(4):
        base = jnp.where(row // 2 == k, labels[k] * 16, base)
    offset = jnp.where(row % 2 == 0, -1, 16)
    pick = jnp.where(((base + offset) & 127) == lane, 1.0, 0.0).astype(BF16)
    picked = pick_dot(pick, edge_ref[...])
    for f in range(FIELDS):
        pick_ref[f * 8 : f * 8 + 8, :] = picked[:, f * LANES : (f + 1) * LANES]
    group = lax.broadcasted_iota(jnp.int32, (5, LANES), 1) // 16
    for n, k in enumerate(DELTAS):
        top = n * HALO
        part = parts[n]
        r = labels[n]

        def put(tile, value):
            shell_ref[tile * 5 : tile * 5 + 5, :] = value

        shell_ref[0:80, :] = part[0:80]
        low = pltpu.roll(pick_ref[pl.ds(n * 2, 5, stride=8), :], (128 - n * 32) % 128, 1)
        high = pltpu.roll(pick_ref[pl.ds(n * 2 + 1, 5, stride=8), :], (192 - n * 32) % 128, 1)
        edge = jnp.where(group < 2, low, jnp.where(group // 2 == 2, high, part[80:85]))
        put(16, edge)
        for q, halo in enumerate((rear_ref, front_ref)):
            for g in range(2):
                near = jnp.zeros((5, LANES), F32)
                far = jnp.zeros((5, LANES), F32)
                for i in range(8):
                    t = top + g * 8 + i
                    shift = ((i - r) & 7) * 16
                    near = jnp.where(
                        group == i, pltpu.roll(halo[pl.ds(t, 5, stride=32), :], shift, 1), near
                    )
                    far = jnp.where(
                        group == i, pltpu.roll(halo[pl.ds(t + 16, 5, stride=32), :], shift, 1), far
                    )
                at = (17 + q * 2 + g) * 5
                put(17 + q * 4 + g, near)
                put(19 + q * 4 + g, (far - part[at : at + 5]) * 0.125)
        corners = (
            rear_ref[top + 160 : top + 165, :],
            rear_ref[top + 168 : top + 173, :],
            front_ref[top + 160 : top + 165, :],
            front_ref[top + 168 : top + 173, :],
        )
        acc = jnp.zeros((5, LANES), F32)
        for c in range(4):
            acc = jnp.where(group == c, pltpu.roll(corners[c], ((c - r) & 7) * 16, 1), acc)
        put(25, acc)
        shell_ref[130:136, :] = jnp.zeros((6, LANES), F32)
        m, place = ROUTES[-k]
        place = 1 if k == -2 else 0
        start = pl.multiple_of(((lev + m) & 3) * (2 * SHELL), 8)
        out_ref[pl.ds(start + place * SHELL, SHELL), :] = shell_ref[...]


EDGES = (
    ((25, 0), (25, 1), (16, 0), (16, 4)),
    ((25, 2), (25, 3), (16, 1), (16, 5)),
    ((25, 0), (25, 2), (16, 2), (16, 6)),
    ((25, 1), (25, 3), (16, 3), (16, 7)),
    ((16, 0), (16, 1), (16, 2), (16, 3)),
    ((16, 4), (16, 5), (16, 6), (16, 7)),
)


def table_kernel(owner_hbm, count_hbm, mask_hbm, base_table, up_table, control_ref,
                 owner_ref, count_ref, mask_ref, sems):
    loads = [
        pltpu.make_async_copy(source, target, sems.at[n])
        for n, (source, target) in enumerate(
            ((owner_hbm, owner_ref), (count_hbm, count_ref), (mask_hbm, mask_ref))
        )
    ]
    for load in loads:
        load.start()
    for chunk in range(8):
        cell = lax.broadcasted_iota(jnp.int32, (384, LANES), 0)
        col = lax.broadcasted_iota(jnp.int32, (384, LANES), 1) + chunk * LANES
        edge = (cell - 256) // 16
        along = cell % 16
        inside = cell < 256
        v = jnp.where(inside, cell // 16, jnp.where(edge == 0, -1, jnp.where(edge == 1, 16, along)))
        w = jnp.where(
            inside, along,
            jnp.where(edge < 2, along, jnp.where(edge == 2, -1, jnp.where(edge == 3, 16, -9))),
        )
        b = col // 32
        c = col % 32
        dv = v - b // 2
        dw = w - c // 2
        sb = jnp.where(b % 2 == 0, -0.125, 0.125)
        sc = jnp.where(c % 2 == 0, -0.125, 0.125)
        along_v = jnp.where(dv == 0, 1.0, jnp.where(dv == 1, sb, jnp.where(dv == -1, -sb, 0.0)))
        along_w = jnp.where(dw == 1, sc, jnp.where(dw == -1, -sc, 0.0))
        table = jnp.where(dw == 0, along_v, jnp.where(dv == 0, along_w, 0.0))
        lanes = slice(chunk * LANES, (chunk + 1) * LANES)
        base_table[:, lanes] = table.astype(BF16)
        up = jnp.where((dv == 0) & (dw == 0), 1.0, 0.0)
        up_table[0:256, lanes] = up[0:256].astype(BF16)
    k_at = lax.broadcasted_iota(jnp.int32, (256, 256), 0)
    n_at = lax.broadcasted_iota(jnp.int32, (256, 256), 1)
    from_y = ((n_at // 32) % 2) * 128 + (n_at // 64) * 32 + n_at % 32
    from_z = (n_at % 2) * 128 + n_at // 2
    up_table[256:512, 0:256] = jnp.where(k_at == from_y, 1.0, 0.0).astype(BF16)
    up_table[256:512, 256:512] = jnp.where(k_at == from_z, 1.0, 0.0).astype(BF16)
    up_table[256:512, 512:1024] = jnp.zeros((256, 512), BF16)
    for load in loads:
        load.wait()
    lev = lax.axis_index("lev")
    row = lax.broadcasted_iota(jnp.int32, (8, LANES), 0)
    for s in range(3):
        k = owner_ref[0, s]
        chosen = jnp.zeros((8, LANES), F32)
        for n, delta in enumerate(DELTAS):
            chosen = jnp.where((row == n) & (k == delta), 1.0, chosen)
        chosen = jnp.where((row == 4) & (((lev + k) & 3) < 2), 1.0, chosen)
        control_ref[s * 8 : s * 8 + 8, :] = chosen
        keep = jnp.zeros((8, LANES), F32)
        for q in range(6):
            keep = jnp.where(
                (row == q) & ((s < count_ref[0, 0]) & (mask_ref[s, q] > 0)), 1.0, keep
            )
        control_ref[24 + s * 8 : 32 + s * 8, :] = keep


def ghost_kernel(control_ref, base_table, up_table, in_ref, out_hbm,
                 shell_ref, plane_ref, spread_ref, out_ref, sems):
    lev = lax.axis_index("lev")
    plane_ref[...] = jnp.zeros_like(plane_ref)
    candidates = []
    for k in DELTAS:
        start = ((lev + k) & 3) * (2 * SHELL) + (SHELL if k == -2 else 0)
        candidates.append(in_ref[pl.ds(pl.multiple_of(start, 8), SHELL), :])
    group = lax.broadcasted_iota(jnp.int32, (5, LANES), 1) // 16
    for s in range(3):
        value = candidates[0]
        for n in range(1, 4):
            row = s * 8 + n
            value = jnp.where(control_ref[row : row + 1, :] > 0.5, candidates[n], value)
        shell_ref[...] = value
        rising = control_ref[s * 8 + 4 : s * 8 + 5, :] > 0.5
        tile = shell_ref[80:85, :]
        swapped = jnp.where(group % 4 == 0, pltpu.roll(tile, 112, 1), pltpu.roll(tile, 16, 1))
        shell_ref[80:85, :] = jnp.where(rising | (group % 4 > 1), tile, swapped)
        tile = shell_ref[125:130, :]
        swapped = jnp.where(group < 2, pltpu.roll(tile, 96, 1), pltpu.roll(tile, 32, 1))
        shell_ref[125:130, :] = jnp.where(rising, tile, swapped)
        for q in range(6):
            def rows(chunk):
                return pl.ds(chunk * 96 + q * 16 + s * 5, 5)

            def tile_at(n):
                if q >= 2:
                    at = ((q - 2) * 4 + n) * 5
                    return shell_ref[at : at + 5, :]
                one, two = ((17 + q * 4 + n) * 5, (21 - q * 4 + n) * 5)
                return jnp.where(rising, shell_ref[one : one + 5, :], shell_ref[two : two + 5, :])

            for g in range(2):
                slope = tile_at(2 + g)
                plane_ref[rows(g), :] = tile_at(g)
                plane_ref[rows(3 + g), :] = slope if q % 2 else -slope
            edges = jnp.zeros((5, LANES), F32)
            for c, (tile, h) in enumerate(EDGES[q]):
                part = shell_ref[tile * 5 : tile * 5 + 5, :]
                shift = ((c - h) % 8) * 16
                if shift:
                    part = pltpu.roll(part, shift, 1)
                edges = jnp.where(group == c, part, edges)
            plane_ref[rows(2), :] = edges

    def chunks(first, count):
        return jnp.concatenate(
            [plane_ref[c * 96 : (c + 1) * 96, :] for c in range(first, first + count)], axis=1
        )

    base = exact_dot(chunks(0, 3), base_table[...])
    slope = exact_dot(chunks(3, 2), up_table[0:256, :])
    lower = base - slope
    upper = base + slope
    keeps = [control_ref[24 + s * 8 : 30 + s * 8, :] > 0.5 for s in range(3)]
    stores = []
    for part in range(4):
        flat = (lower, upper)[part // 2]
        for q in range(2):
            for c in range(4):
                at = (part % 2) * 4 + c
                spread_ref[pl.ds(c * 8 + q, 15, stride=32), :] = flat[
                    q * 16 : q * 16 + 15, at * LANES : (at + 1) * LANES
                ]
        for first in (2, 4):
            top = first * 16
            both = []
            for m in range(part * 2, part * 2 + 2):
                lanes = slice(m * LANES, (m + 1) * LANES)
                both.append(
                    jnp.concatenate([lower[top : top + 32, lanes], upper[top : top + 32, lanes]], axis=1)
                )
            value = exact_dot(
                jnp.concatenate(both, axis=0), up_table[256:512, (first - 2) * 128 : first * 128]
            )
            for q in range(2):
                for c in range(4):
                    row = (c // 2) * 32 + q * 16
                    lanes = slice((c % 2) * LANES, (c % 2 + 1) * LANES)
                    spread_ref[pl.ds(c * 8 + first + q, 15, stride=32), :] = value[row : row + 15, lanes]
        for s in range(3):
            for f in range(FIELDS):
                for c in range(4):
                    row = (s * 5 + f) * 32 + c * 8
                    lanes = slice((part * 4 + c) * LANES, (part * 4 + c + 1) * LANES)
                    out_ref[s, f, :, lanes] = jnp.where(keeps[s], spread_ref[row : row + 6, :], 0.0)
        lanes = pl.ds(part * 512, 512)
        store = pltpu.make_async_copy(
            out_ref.at[:, :, :, lanes], out_hbm.at[:, :, :, lanes], sems.at[part]
        )
        store.start()
        stores.append(store)
    for store in stores:
        store.wait()


def vmem():
    return pl.BlockSpec(memory_space=pltpu.VMEM)


def hbm():
    return pl.BlockSpec(memory_space=pltpu.HBM)


def rows_of(n):
    return jax.ShapeDtypeStruct((n, LANES), F32)


def row_shift(array, by, upper_rises):
    rows, levs = (lax.axis_size("box"), lax.axis_size("lev"))
    pairs = []
    for b in range(rows):
        for v in range(levs):
            way = by if (v >= levs // 2) == upper_rises else -by
            pairs.append((b * levs + v, (b + way) % rows * levs + v))
    return lax.ppermute(array, ("box", "lev"), pairs)


def body(fine, coarse, owner_map, patch_count, face_mask):
    both = ("box", "lev")
    fine = fine.reshape(480, 1024)
    coarse_rows = coarse.reshape(1280, LANES)
    owners = owner_map.T
    counts = patch_count.reshape(1, 1)
    params = pltpu.CompilerParams(vmem_limit_bytes=16 << 20)
    own, leaving = pl.pallas_call(
        restrict_kernel,
        compiler_params=pltpu.CompilerParams(vmem_limit_bytes=K1_VMEM),
        in_specs=[hbm()] * 3,
        out_specs=[vmem()] * 2,
        out_shape=[rows_of(4 * PACK + 32), rows_of(2 * PACK + 8)],
        scratch_shapes=[
            pltpu.VMEM((8 * 480, LANES), F32),
            pltpu.SMEM((2, 3), jnp.int32),
            pltpu.SMEM((1, 1), jnp.int32),
            pltpu.SemaphoreType.DMA((10,)),
        ],
    )(owners, counts, fine)
    arriving = row_shift(leaving, 1, True)
    base_table, up_table, control = pl.pallas_call(
        table_kernel,
        compiler_params=params,
        in_specs=[hbm()] * 3,
        out_specs=[vmem()] * 3,
        out_shape=[
            jax.ShapeDtypeStruct((384, 1024), BF16),
            jax.ShapeDtypeStruct((512, 1024), BF16),
            rows_of(48),
        ],
        scratch_shapes=[
            pltpu.SMEM((2, 3), jnp.int32),
            pltpu.SMEM((1, 1), jnp.int32),
            pltpu.SMEM((3, 6), jnp.int32),
            pltpu.SemaphoreType.DMA((3,)),
        ],
    )(owners, counts, face_mask)
    message = pl.pallas_call(
        message_kernel,
        compiler_params=params,
        in_specs=[vmem()] * 4,
        out_specs=vmem(),
        out_shape=rows_of(4 * MESSAGE),
    )(own, arriving, coarse_rows, control)
    received = lax.all_to_all(message.reshape(4, MESSAGE, LANES), "lev", 0, 0)
    updated, back, back2, ahead, parts = pl.pallas_call(
        place_kernel,
        compiler_params=params,
        in_specs=[vmem()] * 2,
        out_specs=[hbm()] + [vmem()] * 4,
        out_shape=[rows_of(n) for n in (1280, HALO + 2 * PART, HALO, HALO, 4 * PART)],
        scratch_shapes=[pltpu.VMEM((n, LANES), F32) for n in (1280, 160, 160, 480)]
        + [pltpu.SemaphoreType.DMA],
    )(received.reshape(4 * MESSAGE, LANES), coarse_rows)
    from_beyond = row_shift(back2, -2, False)
    from_ahead = row_shift(back, -1, False)
    from_behind = row_shift(ahead, 1, False)
    shells = pl.pallas_call(
        shell_kernel,
        compiler_params=params,
        in_specs=[vmem()] * 5,
        out_specs=vmem(),
        out_shape=rows_of(8 * SHELL),
        scratch_shapes=[
            pltpu.VMEM((n, LANES), F32) for n in (4 * HALO, 4 * HALO, 640, 40, SHELL)
        ],
    )(parts, ahead, from_behind, from_ahead, from_beyond)
    returned = lax.all_to_all(shells.reshape(4, 2 * SHELL, LANES), "lev", 0, 0)
    ghost = pl.pallas_call(
        ghost_kernel,
        compiler_params=params,
        in_specs=[vmem()] * 4,
        out_specs=hbm(),
        out_shape=jax.ShapeDtypeStruct((3, FIELDS, 6, 2048), F32),
        scratch_shapes=[
            pltpu.VMEM((SHELL, LANES), F32),
            pltpu.VMEM((480, LANES), F32),
            pltpu.VMEM((480, LANES), F32),
            pltpu.VMEM((3, FIELDS, 6, 2048), F32),
            pltpu.SemaphoreType.DMA((4,)),
        ],
    )(control, base_table, up_table, returned.reshape(8 * SHELL, LANES))
    ghost = jnp.transpose(ghost, (0, 2, 1, 3))
    return (updated.reshape(coarse.shape), ghost)


def solution(mesh):
    return jax.shard_map(
        body,
        mesh=mesh,
        in_specs=(
            P(("box", "lev"), None, None, None),
            P(None, "box", "lev", None),
            P(("box", "lev"), None),
            P(("box", "lev")),
            P(("box", "lev"), None),
        ),
        out_specs=(P(None, "box", "lev", None), P(("box", "lev"), None, None, None)),
        check_vma=False,
    )
```

```python
import functools

import jax
import jax.numpy as jnp
from jax import lax
from jax.experimental import pallas as pl
from jax.experimental.pallas import tpu as pltpu
from jax.sharding import PartitionSpec as P


DELTAS = (-2, -1, 1, 2)
FIELDS = 5
E = 16
LANES = 128
PACK = 160
SHELL = 136
K1_VMEM = (64 << 20) - 12000000
F32 = jnp.float32
BF16 = jnp.bfloat16


def split(x):
    hi = x.astype(BF16)
    lo = (x - hi.astype(F32)).astype(BF16)
    return hi, lo


def exact_dot(x, table):
    result = jnp.dot(jnp.concatenate(split(x), axis=0), table, preferred_element_type=F32)
    return result[: x.shape[0]] + result[x.shape[0] :]


def carried_by(lev):
    return {-2: lev < 2, -1: lev == 0, 1: lev == 3, 2: lev >= 2}


def restrict_kernel(owner_hbm, count_hbm, fine_hbm, own_ref, carry_ref,
                    fine_ref, owner_ref, count_ref, sems):
    loads = [
        pltpu.make_async_copy(
            fine_hbm.at[:, pl.ds(c * LANES, LANES)], fine_ref.at[pl.ds(c * 480, 480)], sems.at[c]
        )
        for c in range(8)
    ]
    small = [
        pltpu.make_async_copy(owner_hbm, owner_ref, sems.at[8]),
        pltpu.make_async_copy(count_hbm, count_ref, sems.at[9]),
    ]
    for copy in small + loads:
        copy.start()
    carried = carried_by(lax.axis_index("lev"))
    own_ref[0 : 4 * PACK, :] = jnp.zeros((4 * PACK, LANES), F32)
    own_ref[4 * PACK : 4 * PACK + 32, :] = jnp.full((32, LANES), -1.0, F32)
    carry_ref[0 : 2 * PACK, :] = jnp.zeros((2 * PACK, LANES), F32)
    carry_ref[2 * PACK : 2 * PACK + 8, :] = jnp.full((8, LANES), -1.0, F32)
    source = lax.broadcasted_iota(jnp.int32, (512, LANES), 0)
    target = lax.broadcasted_iota(jnp.int32, (512, LANES), 1)
    table = jnp.where((source // 64) * 16 + (source % 32) // 2 == target, 0.125, 0.0).astype(BF16)
    for copy in small:
        copy.wait()
    for g in range(2):
        packed = jnp.zeros((240, LANES), F32)
        for h in range(2):
            pairs = []
            for c in range(g * 4 + h * 2, g * 4 + h * 2 + 2):
                loads[c].wait()
                at = c * 480
                pairs.append(
                    fine_ref[pl.ds(at, 240, stride=2), :] + fine_ref[pl.ds(at + 1, 240, stride=2), :]
                )
            packed += exact_dot(
                jnp.concatenate(pairs, axis=1), table[h * 256 : (h + 1) * 256]
            )
        for s in range(3):
            live = s < count_ref[0, 0]
            offset = owner_ref[0, s]
            part = packed[s * 80 : s * 80 + 80]
            for n, delta in enumerate(DELTAS):
                here = live & (offset == delta)
                at = 0 if abs(delta) == 2 else 1

                @pl.when(here & carried[delta])
                def _():
                    row = at * PACK + g * 80
                    carry_ref[row : row + 80, :] = part
                    if g == 0:
                        row = 2 * PACK + at * 4
                        region = owner_ref[1, s].astype(F32)
                        carry_ref[row : row + 4, :] = jnp.full((4, LANES), region, F32)

                @pl.when(here & jnp.logical_not(carried[delta]))
                def _():
                    row = n * PACK + g * 80
                    own_ref[row : row + 80, :] = part
                    if g == 0:
                        row = 4 * PACK + n * 8
                        region = owner_ref[1, s].astype(F32)
                        own_ref[row : row + 8, :] = jnp.full((8, LANES), region, F32)


PIECES = (((1, 0), (-1, 1)), ((2, 0), (-2, 0)), ((-1, 0), (1, 1)), ((2, 1), (-2, 1)))
ROUTES = {1: (1, 0), -1: (3, 0), 2: (2, 0), -2: (2, 1)}
MESSAGE = 368


def message_kernel(own_ref, carry_ref, coarse_ref, control_ref, out_ref):
    lev = lax.axis_index("lev")
    carried = carried_by(lev)
    lane = lax.broadcasted_iota(jnp.int32, (8, LANES), 1)
    row8 = lax.broadcasted_iota(jnp.int32, (8, LANES), 0)
    carry_labels = carry_ref[2 * PACK : 2 * PACK + 8, :]
    data = {}
    label = {}
    for n, k in enumerate(DELTAS):
        at = 0 if abs(k) == 2 else 1
        data[k] = jnp.where(
            carried[k],
            carry_ref[at * PACK : (at + 1) * PACK, :],
            own_ref[n * PACK : (n + 1) * PACK, :],
        )
        row = 4 * PACK + n * 8
        label[k] = jnp.where(
            carried[k],
            jnp.max(jnp.where(row8 // 4 == at, carry_labels, -1.0), axis=0, keepdims=True),
            own_ref[row : row + 1, :],
        )
    starts = [pl.multiple_of(((lev + m) & 3) * MESSAGE, 8) for m in range(4)]
    for k in DELTAS:
        m, place = ROUTES[k]
        out_ref[pl.ds(starts[m] + place * PACK, PACK), :] = data[k]
    for m, layers in ((1, (15, 14)), (3, (0, 1))):
        for d, y in enumerate(layers):
            out_ref[pl.ds(starts[m] + PACK + d * 80, 80), :] = coarse_ref[pl.ds(y, 80, stride=16), :]
    none = jnp.full((1, LANES), -1.0, F32)
    wide = lax.broadcasted_iota(jnp.int32, (80, LANES), 1)
    for m in range(4):
        parts = []
        for n, (k, high) in enumerate(PIECES[m]):
            rows = data[k][80:160] if high else data[k][0:80]
            shift = 32 * (n + high)
            parts.append(pltpu.roll(rows, shift, 1) if shift else rows)
        tile = jnp.where(wide < 32, parts[0], parts[1])
        for f in range(FIELDS):
            near = tile[f * 16 : f * 16 + 8]
            far = pltpu.roll(tile[f * 16 + 8 : f * 16 + 16], 64, 1)
            out_ref[pl.ds(starts[m] + 320 + f * 8, 8), :] = jnp.where(lane < 64, near, far)
        first = label[1] if m == 1 else label[2] if m == 2 else label[-1] if m == 3 else none
        second = label[-2] if m == 2 else none
        k0, k1 = PIECES[m][0][0], PIECES[m][1][0]
        out_ref[pl.ds(starts[m] + 360, 8), :] = jnp.where(
            row8 < 2, first, jnp.where(row8 < 4, second, jnp.where(row8 < 6, label[k0], label[k1]))
        )


PART = 112
HALO = 176
NT = (((1,), (1,)), ((), ()))


def pick_dot(pick, rows):
    hi, lo = split(rows)
    return lax.dot_general(pick, hi, NT, preferred_element_type=F32) + lax.dot_general(
        pick, lo, NT, preferred_element_type=F32
    )


def place_kernel(in_ref, coarse_ref, upd_hbm, back_ref, back2_ref, fwd_ref, part_ref,
                 upd_ref, yl_ref, yh_ref, z_ref, sem):
    lev = lax.axis_index("lev")
    rising = lev < 2
    starts = [pl.multiple_of(((lev - m) & 3) * MESSAGE, 8) for m in range(4)]
    row8 = lax.broadcasted_iota(jnp.int32, (8, LANES), 0)
    heads = [in_ref[pl.ds(starts[m] + 360, 8), :] for m in range(4)]

    def label(m, n):
        return jnp.max(jnp.where(row8 // 2 == n, heads[m], -1.0)).astype(jnp.int32)

    group = lax.broadcasted_iota(jnp.int32, (80, LANES), 1) // 16
    labels = [label(*ROUTES[k]) for k in DELTAS]
    masks = [group == r for r in labels]
    for g in range(2):
        arrived = [
            in_ref[pl.ds(starts[ROUTES[k][0]] + ROUTES[k][1] * PACK + g * 80, 80), :] for k in DELTAS
        ]
        for i in range(8):
            rows = pl.ds(g * 8 + i, 80, stride=16)
            acc = coarse_ref[rows, :]
            for a, r, m in zip(arrived, labels, masks):
                acc = jnp.where(m, pltpu.roll(a, ((r - i) & 7) * 16, 1), acc)
            upd_ref[rows, :] = acc
    store = pltpu.make_async_copy(upd_ref, upd_hbm, sem)
    store.start()

    @pl.when(lev < 4)
    def _():
        for out, m_coarse, found in (
            (yl_ref, 1, ((0, 1), (2, 1), (3, 0), (3, 1))),
            (yh_ref, 3, ((0, 0), (2, 0), (1, 0), (1, 1))),
        ):
            high = out is yl_ref
            pieces = [(in_ref[pl.ds(starts[m] + 320, 40), :], n, label(m, n + 2)) for m, n in found]
            for d in range(2):
                halo = in_ref[pl.ds(starts[m_coarse] + PACK + d * 80, 80), :]
                for tile, n, r in pieces:
                    first = n * 2 + (1 - d if high else d)
                    halves = [
                        pltpu.roll(tile, ((r - first - h * 4) & 7) * 16, 1) for h in range(2)
                    ]
                    rows = []
                    for f in range(FIELDS):
                        for h in range(2):
                            rows.append(halves[h][f * 8 : f * 8 + 8])
                    halo = jnp.where(group == r, jnp.concatenate(rows, axis=0), halo)
                out[d * 80 : d * 80 + 80, :] = halo
        for out, low in ((back2_ref, True), (fwd_ref, False)):
            at_low = rising if low else jnp.logical_not(rising)
            for f in range(FIELDS):
                for d in range(2):
                    one = upd_ref[f * 256 + d * 16 : f * 256 + d * 16 + 16, :]
                    two = upd_ref[f * 256 + 240 - d * 16 : f * 256 + 256 - d * 16, :]
                    out[f * 32 + d * 16 : f * 32 + d * 16 + 16, :] = jnp.where(at_low, one, two)
            out[160:176, :] = jnp.zeros((16, LANES), F32)
            for row, side in ((160, yl_ref), (168, yh_ref)):
                out[row : row + 5, :] = jnp.where(
                    at_low, side[pl.ds(0, 5, stride=16), :], side[pl.ds(15, 5, stride=16), :]
                )
        row = lax.broadcasted_iota(jnp.int32, (32, LANES), 0)
        lane = lax.broadcasted_iota(jnp.int32, (32, LANES), 1)
        layer = row % 6
        offset = jnp.where(layer < 3, layer - 2, layer + 12)
        base = jnp.zeros_like(row)
        for k in range(4):
            base = jnp.where(row // 6 == k, labels[k] * 16, base)
        pick = jnp.where((row < 24) & (((base + offset) & 127) == lane), 1.0, 0.0).astype(BF16)
        for f in range(FIELDS):
            rows = jnp.concatenate(
                [
                    upd_ref[f * 256 : f * 256 + 256, :],
                    yl_ref[f * 16 : f * 16 + 16, :],
                    yh_ref[f * 16 : f * 16 + 16, :],
                ],
                axis=0,
            )
            picked = pick_dot(pick, rows)
            for c, width in enumerate((LANES, LANES, 32)):
                at = c * 160 + f * 32
                z_ref[at : at + 32, 0:width] = picked[:, c * LANES : c * LANES + width]
        strip = lax.broadcasted_iota(jnp.int32, (5, LANES), 1) // 16

        def put(k, tile, value):
            at = k * PART + tile * 5
            part_ref[at : at + 5, :] = value

        for k in range(4):
            for g in range(2):
                plane = [z_ref[pl.ds(g * 160 + k * 6 + n, 5, stride=32), :] for n in range(6)]
                put(k, 8 + g, plane[1])
                put(k, 10 + g, (plane[0] - plane[2]) * 0.125)
                put(k, 12 + g, plane[4])
                put(k, 14 + g, (plane[5] - plane[3]) * 0.125)
            first = pltpu.roll(z_ref[pl.ds(320 + k * 6 + 1, 5, stride=32), :], 32, 1)
            last = pltpu.roll(z_ref[pl.ds(320 + k * 6 + 4, 5, stride=32), :], 96, 1)
            edge = jnp.where(strip // 2 == 1, first, jnp.where(strip // 2 == 3, last, 0.0))
            put(k, 16, edge)
            at = k * PART + 105
            part_ref[at : at + 7, :] = jnp.full((7, LANES), labels[k].astype(F32), F32)
        for q in range(2):
            side = yh_ref if q else yl_ref
            facing = fwd_ref if q else back2_ref
            for g in range(2):
                accs = [[jnp.zeros((5, LANES), F32)] * 3 for _ in range(4)]
                for i in range(8):
                    t = g * 8 + i
                    near = side[pl.ds(t, 5, stride=16), :]
                    far = side[pl.ds(80 + t, 5, stride=16), :]
                    inner = upd_ref[pl.ds(t * 16 + q * 15, 5, stride=256), :]
                    values = (near, (far - inner) * 0.125, facing[pl.ds(t, 5, stride=32), :])
                    for k in range(4):
                        shift = ((i - labels[k]) & 7) * 16
                        accs[k] = [
                            jnp.where(strip == i, pltpu.roll(v, shift, 1), a)
                            for v, a in zip(values, accs[k])
                        ]
                for k in range(4):
                    put(k, q * 4 + g, accs[k][0])
                    put(k, q * 4 + 2 + g, accs[k][1])
                    put(k, 17 + q * 2 + g, accs[k][2])
        back_ref[0:HALO, :] = back2_ref[...]
        for c, (up, down) in enumerate(((3, 0), (2, 1))):
            back_ref[HALO + c * PART : HALO + (c + 1) * PART, :] = jnp.where(
                rising,
                part_ref[up * PART : (up + 1) * PART, :],
                part_ref[down * PART : (down + 1) * PART, :],
            )

    store.wait()


def shell_kernel(part_ref, mine_ref, behind_ref, ahead_ref, beyond_ref, out_ref,
                 rear_ref, front_ref, edge_ref, pick_ref, shell_ref):
    lev = lax.axis_index("lev")
    rising = lev < 2
    falling = jnp.logical_not(rising)
    returned = (falling, lev == 3, lev == 0, rising)
    parts = []
    labels = []
    for n, k in enumerate(DELTAS):
        at = HALO + (0 if abs(k) == 2 else 1) * PART
        part = jnp.where(
            returned[n], ahead_ref[at : at + PART, :], part_ref[n * PART : (n + 1) * PART, :]
        )
        parts.append(part)
        labels.append(jnp.maximum(jnp.max(part[105:112]), 0.0).astype(jnp.int32))
        top = n * HALO
        rear_ref[top : top + HALO, :] = jnp.where(returned[n], mine_ref[...], behind_ref[...])
        front_ref[top : top + HALO, :] = jnp.where(
            returned[n], beyond_ref[...], ahead_ref[0:HALO, :]
        )
        for f in range(FIELDS):
            at = f * 128 + n * 32
            edge_ref[at : at + 16, :] = rear_ref[top + f * 32 : top + f * 32 + 16, :]
            edge_ref[at + 16 : at + 32, :] = front_ref[top + f * 32 : top + f * 32 + 16, :]
    row = lax.broadcasted_iota(jnp.int32, (8, LANES), 0)
    lane = lax.broadcasted_iota(jnp.int32, (8, LANES), 1)
    base = jnp.zeros_like(row)
    for k in range(4):
        base = jnp.where(row // 2 == k, labels[k] * 16, base)
    offset = jnp.where(row % 2 == 0, -1, 16)
    pick = jnp.where(((base + offset) & 127) == lane, 1.0, 0.0).astype(BF16)
    picked = pick_dot(pick, edge_ref[...])
    for f in range(FIELDS):
        pick_ref[f * 8 : f * 8 + 8, :] = picked[:, f * LANES : (f + 1) * LANES]
    group = lax.broadcasted_iota(jnp.int32, (5, LANES), 1) // 16
    for n, k in enumerate(DELTAS):
        top = n * HALO
        part = parts[n]
        r = labels[n]

        def put(tile, value):
            shell_ref[tile * 5 : tile * 5 + 5, :] = value

        shell_ref[0:80, :] = part[0:80]
        low = pltpu.roll(pick_ref[pl.ds(n * 2, 5, stride=8), :], (128 - n * 32) % 128, 1)
        high = pltpu.roll(pick_ref[pl.ds(n * 2 + 1, 5, stride=8), :], (192 - n * 32) % 128, 1)
        edge = jnp.where(group < 2, low, jnp.where(group // 2 == 2, high, part[80:85]))
        put(16, edge)
        for q, halo in enumerate((rear_ref, front_ref)):
            for g in range(2):
                near = jnp.zeros((5, LANES), F32)
                far = jnp.zeros((5, LANES), F32)
                for i in range(8):
                    t = top + g * 8 + i
                    shift = ((i - r) & 7) * 16
                    near = jnp.where(
                        group == i, pltpu.roll(halo[pl.ds(t, 5, stride=32), :], shift, 1), near
                    )
                    far = jnp.where(
                        group == i, pltpu.roll(halo[pl.ds(t + 16, 5, stride=32), :], shift, 1), far
                    )
                at = (17 + q * 2 + g) * 5
                put(17 + q * 4 + g, near)
                put(19 + q * 4 + g, (far - part[at : at + 5]) * 0.125)
        corners = (
            rear_ref[top + 160 : top + 165, :],
            rear_ref[top + 168 : top + 173, :],
            front_ref[top + 160 : top + 165, :],
            front_ref[top + 168 : top + 173, :],
        )
        acc = jnp.zeros((5, LANES), F32)
        for c in range(4):
            acc = jnp.where(group == c, pltpu.roll(corners[c], ((c - r) & 7) * 16, 1), acc)
        put(25, acc)
        shell_ref[130:136, :] = jnp.zeros((6, LANES), F32)
        m, place = ROUTES[-k]
        place = 1 if k == -2 else 0
        start = pl.multiple_of(((lev + m) & 3) * (2 * SHELL), 8)
        out_ref[pl.ds(start + place * SHELL, SHELL), :] = shell_ref[...]


EDGES = (
    ((25, 0), (25, 1), (16, 0), (16, 4)),
    ((25, 2), (25, 3), (16, 1), (16, 5)),
    ((25, 0), (25, 2), (16, 2), (16, 6)),
    ((25, 1), (25, 3), (16, 3), (16, 7)),
    ((16, 0), (16, 1), (16, 2), (16, 3)),
    ((16, 4), (16, 5), (16, 6), (16, 7)),
)


def table_kernel(owner_hbm, count_hbm, mask_hbm, base_table, up_table, control_ref,
                 owner_ref, count_ref, mask_ref, sems):
    loads = [
        pltpu.make_async_copy(source, target, sems.at[n])
        for n, (source, target) in enumerate(
            ((owner_hbm, owner_ref), (count_hbm, count_ref), (mask_hbm, mask_ref))
        )
    ]
    for load in loads:
        load.start()
    for chunk in range(8):
        cell = lax.broadcasted_iota(jnp.int32, (384, LANES), 0)
        col = lax.broadcasted_iota(jnp.int32, (384, LANES), 1) + chunk * LANES
        edge = (cell - 256) // 16
        along = cell % 16
        inside = cell < 256
        v = jnp.where(inside, cell // 16, jnp.where(edge == 0, -1, jnp.where(edge == 1, 16, along)))
        w = jnp.where(
            inside, along,
            jnp.where(edge < 2, along, jnp.where(edge == 2, -1, jnp.where(edge == 3, 16, -9))),
        )
        b = col // 32
        c = col % 32
        dv = v - b // 2
        dw = w - c // 2
        sb = jnp.where(b % 2 == 0, -0.125, 0.125)
        sc = jnp.where(c % 2 == 0, -0.125, 0.125)
        along_v = jnp.where(dv == 0, 1.0, jnp.where(dv == 1, sb, jnp.where(dv == -1, -sb, 0.0)))
        along_w = jnp.where(dw == 1, sc, jnp.where(dw == -1, -sc, 0.0))
        table = jnp.where(dw == 0, along_v, jnp.where(dv == 0, along_w, 0.0))
        lanes = slice(chunk * LANES, (chunk + 1) * LANES)
        base_table[:, lanes] = table.astype(BF16)
        up = jnp.where((dv == 0) & (dw == 0), 1.0, 0.0)
        up_table[0:256, lanes] = up[0:256].astype(BF16)
    k_at = lax.broadcasted_iota(jnp.int32, (256, 256), 0)
    n_at = lax.broadcasted_iota(jnp.int32, (256, 256), 1)
    from_y = ((n_at // 32) % 2) * 128 + (n_at // 64) * 32 + n_at % 32
    from_z = (n_at % 2) * 128 + n_at // 2
    up_table[256:512, 0:256] = jnp.where(k_at == from_y, 1.0, 0.0).astype(BF16)
    up_table[256:512, 256:512] = jnp.where(k_at == from_z, 1.0, 0.0).astype(BF16)
    up_table[256:512, 512:1024] = jnp.zeros((256, 512), BF16)
    for load in loads:
        load.wait()
    lev = lax.axis_index("lev")
    row = lax.broadcasted_iota(jnp.int32, (8, LANES), 0)
    for s in range(3):
        k = owner_ref[0, s]
        chosen = jnp.zeros((8, LANES), F32)
        for n, delta in enumerate(DELTAS):
            chosen = jnp.where((row == n) & (k == delta), 1.0, chosen)
        chosen = jnp.where((row == 4) & (((lev + k) & 3) < 2), 1.0, chosen)
        control_ref[s * 8 : s * 8 + 8, :] = chosen
        keep = jnp.zeros((8, LANES), F32)
        for q in range(6):
            keep = jnp.where(
                (row == q) & ((s < count_ref[0, 0]) & (mask_ref[s, q] > 0)), 1.0, keep
            )
        control_ref[24 + s * 8 : 32 + s * 8, :] = keep


def ghost_kernel(control_ref, base_table, up_table, in_ref, out_hbm,
                 shell_ref, plane_ref, spread_ref, out_ref, sems):
    lev = lax.axis_index("lev")
    plane_ref[...] = jnp.zeros_like(plane_ref)
    candidates = []
    for k in DELTAS:
        start = ((lev + k) & 3) * (2 * SHELL) + (SHELL if k == -2 else 0)
        candidates.append(in_ref[pl.ds(pl.multiple_of(start, 8), SHELL), :])
    group = lax.broadcasted_iota(jnp.int32, (5, LANES), 1) // 16
    for s in range(3):
        value = candidates[0]
        for n in range(1, 4):
            row = s * 8 + n
            value = jnp.where(control_ref[row : row + 1, :] > 0.5, candidates[n], value)
        shell_ref[...] = value
        rising = control_ref[s * 8 + 4 : s * 8 + 5, :] > 0.5
        tile = shell_ref[80:85, :]
        swapped = jnp.where(group % 4 == 0, pltpu.roll(tile, 112, 1), pltpu.roll(tile, 16, 1))
        shell_ref[80:85, :] = jnp.where(rising | (group % 4 > 1), tile, swapped)
        tile = shell_ref[125:130, :]
        swapped = jnp.where(group < 2, pltpu.roll(tile, 96, 1), pltpu.roll(tile, 32, 1))
        shell_ref[125:130, :] = jnp.where(rising, tile, swapped)
        for q in range(6):
            def rows(chunk):
                return pl.ds(chunk * 96 + q * 16 + s * 5, 5)

            def tile_at(n):
                if q >= 2:
                    at = ((q - 2) * 4 + n) * 5
                    return shell_ref[at : at + 5, :]
                one, two = ((17 + q * 4 + n) * 5, (21 - q * 4 + n) * 5)
                return jnp.where(rising, shell_ref[one : one + 5, :], shell_ref[two : two + 5, :])

            for g in range(2):
                slope = tile_at(2 + g)
                plane_ref[rows(g), :] = tile_at(g)
                plane_ref[rows(3 + g), :] = slope if q % 2 else -slope
            edges = jnp.zeros((5, LANES), F32)
            for c, (tile, h) in enumerate(EDGES[q]):
                part = shell_ref[tile * 5 : tile * 5 + 5, :]
                shift = ((c - h) % 8) * 16
                if shift:
                    part = pltpu.roll(part, shift, 1)
                edges = jnp.where(group == c, part, edges)
            plane_ref[rows(2), :] = edges

    def chunks(first, count):
        return jnp.concatenate(
            [plane_ref[c * 96 : (c + 1) * 96, :] for c in range(first, first + count)], axis=1
        )

    base = exact_dot(chunks(0, 3), base_table[...])
    slope = exact_dot(chunks(3, 2), up_table[0:256, :])
    lower = base - slope
    upper = base + slope
    keeps = [control_ref[24 + s * 8 : 30 + s * 8, :] > 0.5 for s in range(3)]
    stores = []
    for part in range(4):
        flat = (lower, upper)[part // 2]
        for q in range(2):
            for c in range(4):
                at = (part % 2) * 4 + c
                spread_ref[pl.ds(c * 8 + q, 15, stride=32), :] = flat[
                    q * 16 : q * 16 + 15, at * LANES : (at + 1) * LANES
                ]
        for first in (2, 4):
            top = first * 16
            both = []
            for m in range(part * 2, part * 2 + 2):
                lanes = slice(m * LANES, (m + 1) * LANES)
                both.append(
                    jnp.concatenate([lower[top : top + 32, lanes], upper[top : top + 32, lanes]], axis=1)
                )
            value = exact_dot(
                jnp.concatenate(both, axis=0), up_table[256:512, (first - 2) * 128 : first * 128]
            )
            for q in range(2):
                for c in range(4):
                    row = (c // 2) * 32 + q * 16
                    lanes = slice((c % 2) * LANES, (c % 2 + 1) * LANES)
                    spread_ref[pl.ds(c * 8 + first + q, 15, stride=32), :] = value[row : row + 15, lanes]
        for s in range(3):
            for f in range(FIELDS):
                for c in range(4):
                    row = (s * 5 + f) * 32 + c * 8
                    lanes = slice((part * 4 + c) * LANES, (part * 4 + c + 1) * LANES)
                    out_ref[s, f, :, lanes] = jnp.where(keeps[s], spread_ref[row : row + 6, :], 0.0)
        lanes = pl.ds(part * 512, 512)
        store = pltpu.make_async_copy(
            out_ref.at[:, :, :, lanes], out_hbm.at[:, :, :, lanes], sems.at[part]
        )
        store.start()
        stores.append(store)
    for store in stores:
        store.wait()


def vmem():
    return pl.BlockSpec(memory_space=pltpu.VMEM)


def hbm():
    return pl.BlockSpec(memory_space=pltpu.HBM)


def rows_of(n):
    return jax.ShapeDtypeStruct((n, LANES), F32)


def row_shift(array, by, upper_rises):
    rows, levs = (lax.axis_size("box"), lax.axis_size("lev"))
    pairs = []
    for b in range(rows):
        for v in range(levs):
            way = by if (v >= levs // 2) == upper_rises else -by
            pairs.append((b * levs + v, (b + way) % rows * levs + v))
    return lax.ppermute(array, ("box", "lev"), pairs)


def body(fine, coarse, owner_map, patch_count, face_mask):
    both = ("box", "lev")
    fine = fine.reshape(480, 1024)
    coarse_rows = coarse.reshape(1280, LANES)
    owners = owner_map.T
    counts = patch_count.reshape(1, 1)
    params = pltpu.CompilerParams(vmem_limit_bytes=16 << 20)
    own, leaving = pl.pallas_call(
        restrict_kernel,
        compiler_params=pltpu.CompilerParams(vmem_limit_bytes=K1_VMEM),
        in_specs=[hbm()] * 3,
        out_specs=[vmem()] * 2,
        out_shape=[rows_of(4 * PACK + 32), rows_of(2 * PACK + 8)],
        scratch_shapes=[
            pltpu.VMEM((8 * 480, LANES), F32),
            pltpu.SMEM((2, 3), jnp.int32),
            pltpu.SMEM((1, 1), jnp.int32),
            pltpu.SemaphoreType.DMA((10,)),
        ],
    )(owners, counts, fine)
    arriving = row_shift(leaving, 1, True)
    base_table, up_table, control = pl.pallas_call(
        table_kernel,
        compiler_params=params,
        in_specs=[hbm()] * 3,
        out_specs=[vmem()] * 3,
        out_shape=[
            jax.ShapeDtypeStruct((384, 1024), BF16),
            jax.ShapeDtypeStruct((512, 1024), BF16),
            rows_of(48),
        ],
        scratch_shapes=[
            pltpu.SMEM((2, 3), jnp.int32),
            pltpu.SMEM((1, 1), jnp.int32),
            pltpu.SMEM((3, 6), jnp.int32),
            pltpu.SemaphoreType.DMA((3,)),
        ],
    )(owners, counts, face_mask)
    message = pl.pallas_call(
        message_kernel,
        compiler_params=params,
        in_specs=[vmem()] * 4,
        out_specs=vmem(),
        out_shape=rows_of(4 * MESSAGE),
    )(own, arriving, coarse_rows, control)
    received = lax.all_to_all(message.reshape(4, MESSAGE, LANES), "lev", 0, 0)
    updated, back, back2, ahead, parts = pl.pallas_call(
        place_kernel,
        compiler_params=params,
        in_specs=[vmem()] * 2,
        out_specs=[hbm()] + [vmem()] * 4,
        out_shape=[rows_of(n) for n in (1280, HALO + 2 * PART, HALO, HALO, 4 * PART)],
        scratch_shapes=[pltpu.VMEM((n, LANES), F32) for n in (1280, 160, 160, 480)]
        + [pltpu.SemaphoreType.DMA],
    )(received.reshape(4 * MESSAGE, LANES), coarse_rows)
    from_beyond = row_shift(back2, -2, False)
    from_ahead = row_shift(back, -1, False)
    from_behind = row_shift(ahead, 1, False)
    shells = pl.pallas_call(
        shell_kernel,
        compiler_params=params,
        in_specs=[vmem()] * 5,
        out_specs=vmem(),
        out_shape=rows_of(8 * SHELL),
        scratch_shapes=[
            pltpu.VMEM((n, LANES), F32) for n in (4 * HALO, 4 * HALO, 640, 40, SHELL)
        ],
    )(parts, ahead, from_behind, from_ahead, from_beyond)
    returned = lax.all_to_all(shells.reshape(4, 2 * SHELL, LANES), "lev", 0, 0)
    ghost = pl.pallas_call(
        ghost_kernel,
        compiler_params=params,
        in_specs=[vmem()] * 4,
        out_specs=hbm(),
        out_shape=jax.ShapeDtypeStruct((3, FIELDS, 6, 2048), F32),
        scratch_shapes=[
            pltpu.VMEM((SHELL, LANES), F32),
            pltpu.VMEM((480, LANES), F32),
            pltpu.VMEM((480, LANES), F32),
            pltpu.VMEM((3, FIELDS, 6, 2048), F32),
            pltpu.SemaphoreType.DMA((4,)),
        ],
    )(control, base_table, up_table, returned.reshape(8 * SHELL, LANES))
    ghost = jnp.transpose(ghost, (0, 2, 1, 3))
    return (updated.reshape(coarse.shape), ghost)


def solution(mesh):
    return jax.shard_map(
        body,
        mesh=mesh,
        in_specs=(
            P(("box", "lev"), None, None, None),
            P(None, "box", "lev", None),
            P(("box", "lev"), None),
            P(("box", "lev")),
            P(("box", "lev"), None),
        ),
        out_specs=(P(None, "box", "lev", None), P(("box", "lev"), None, None, None)),
        check_vma=False,
    )
```
